32 devices in a mesh: dp: 16 (over z, x, core), tensor: 2 (over y).
Axes of the slice: x: 2, y: 2, z: 4, core: 2. Of those that a mesh axis runs over, the one named last changes fastest.
Arguments:
- tokens: bfloat16 [32768, 512], P(('dp', 'tensor')), may hold values from -6 to 6
- cotangent: bfloat16 [32768, 512], P(('dp', 'tensor')), may hold values from -6 to 6
- w_qkv: bfloat16 [512, 3, 512], P(None, None, 'tensor'), may hold values from -0.25 to 0.25
- w_out: bfloat16 [512, 512], P('tensor'), may hold values from -1.5 to 1.5
- w_up: bfloat16 [512, 2048], P(None, 'tensor'), may hold values from -0.25 to 0.25
- w_down: bfloat16 [2048, 512], P('tensor'), may hold values from -0.125 to 0.125
- gains: float32 [2, 512], replicated, may hold values from 0.25 to 1.75
- shifts: float32 [2, 512], replicated, may hold values from -3 to 3
- feat_fresh: bfloat16 [64, 256], replicated, may hold values from -5 to 5
- feat_last: bfloat16 [64, 256], replicated, may hold values from -5 to 5
- flags: int32 [8], replicated, may hold values from 0 to 1, as said below
Outputs:
- block_out: float32 [32768, 512], P(('dp', 'tensor'))
- grad_tokens: float32 [32768, 512], P(('dp', 'tensor'))
- grad_qkv: float32 [512, 3, 512], P('dp', None, 'tensor')
- grad_wout: float32 [512, 512], P('tensor', 'dp')
- grad_up: float32 [512, 2048], P('dp', 'tensor')
- grad_down: float32 [2048, 512], P('tensor', 'dp')
- grad_gains: float32 [2, 512], replicated
- grad_shifts: float32 [2, 512], replicated
The draws below stay inside these ranges and needn't reach their ends.
Inputs may be any that keep to these rules, and one draw needn't show every extreme that they name: `flags`: exactly half of the 8 heads take the fresh matrix.
All inputs are finite; a program needn't handle non-finite values.
Results may differ from the reference program's by a relative error of at most 0.029.
Values may be sent and summed in bfloat16 or wider, within the bound.
A program may use at most 192 MiB of HBM per device.

```python
import jax
import jax.numpy as jnp
from jax import lax

D = 512
HEADS = 8
HEAD_DIM = 64
FEATURES = 256
FF = 2048
BLOCK = 1024
SEQ_LEN = 2048
SEQS = 16
TOKENS = 32768


def draw_flags(key, part):
    order = jax.random.permutation(key, HEADS)
    return (order % 2).astype(jnp.int32)


def shard_levels(rng, extent, cuts, smallest, high):
    loudness = 1.0
    for axis_at, blocks in cuts:
        heights = jax.random.uniform(jax.random.fold_in(jax.random.fold_in(rng, 6), axis_at), (blocks,), jnp.float32, smallest / len(cuts), high / len(cuts))
        loudness = loudness * jnp.repeat(jnp.exp(heights), extent[axis_at] // blocks).reshape((-1,) + (1,) * (len(extent) - 1 - axis_at))
    return loudness


def gaussian(key, shape, scale, bound, split=(), held_as=jnp.bfloat16):
    values = jax.random.normal(key, shape, jnp.float32) * scale
    if len(split) > 0:
        values = shard_levels(key, shape, split, -0.22, 0.18) * values
    return jnp.clip(values, min=-bound, max=bound).astype(held_as)


def setup_inputs(seed: int = 0) -> dict:
    streams_of = jax.random.split(jax.random.key(seed), 12)
    tokens = gaussian(streams_of[0], (TOKENS, D), 1.0, 6.0, ((0, 32),))
    cotangent = gaussian(streams_of[1], (TOKENS, D), 1.0, 6.0, ((0, 32),))
    w_qkv = gaussian(streams_of[2], (D, 3, D), D ** -0.5, 0.25, ((2, 2),))
    w_out = gaussian(streams_of[3], (D, D), (D // 32) ** -0.5, 1.5, ((0, 2),))
    w_up = gaussian(streams_of[4], (D, FF), D ** -0.5, 0.25, ((1, 2),))
    w_down = gaussian(streams_of[5], (FF, D), FF ** -0.5, 0.125, ((0, 2),))
    gains = jnp.clip(1.0 + 0.15 * jax.random.normal(streams_of[6], (2, D), jnp.float32), 0.25, 1.75)
    shifts = gaussian(streams_of[7], (2, D), 0.5, 3.0, (), jnp.float32)
    feat_fresh = gaussian(streams_of[8], (HEAD_DIM, FEATURES), 1.0, 5.0)
    feat_last = gaussian(streams_of[9], (HEAD_DIM, FEATURES), 1.0, 5.0)
    flags = draw_flags(jax.random.fold_in(streams_of[11], 71), 0)
    return dict(tokens=tokens, cotangent=cotangent, w_qkv=w_qkv, w_out=w_out, w_up=w_up, w_down=w_down, gains=gains, shifts=shifts, feat_fresh=feat_fresh, feat_last=feat_last, flags=flags)


HIGH = lax.Precision.HIGHEST
EPS = 1e-05

@jax.custom_vjp
def low(v):
    return lax.optimization_barrier(v.astype(jnp.bfloat16)).astype(jnp.float32)

@jax.custom_vjp
def low_back(v):
    return v

def low_keep(v):
    return (low(v), None)

def low_pass(kept, grad):
    return (grad,)

def back_keep(v):
    return (v, None)

def back_low(kept, grad):
    return (low(grad),)
low.defvjp(low_keep, low_pass)
low_back.defvjp(back_keep, back_low)

def normalize(inputs, norm_gain, offset):
    average = lax.optimization_barrier(jnp.mean(inputs, axis=-1, keepdims=True))
    centered = inputs - average
    variance = lax.optimization_barrier(jnp.mean(centered * centered, axis=-1, keepdims=True))
    return centered * lax.rsqrt(variance + EPS) * norm_gain + offset

def head_features(inputs, projector):
    factor = HEAD_DIM ** (-0.25)
    projected = low_back(jnp.dot(inputs, projector, precision=HIGH))
    squares = 0.5 * factor * factor * lax.optimization_barrier(jnp.sum(inputs * inputs, axis=-1, keepdims=True))
    return low(jnp.exp(factor * projected - squares) * FEATURES ** (-0.5))

def head_attention(queries, key_rows, values, projector):
    length = queries.shape[0]
    blocks = length // BLOCK
    phi_q = head_features(queries, projector).reshape(blocks, BLOCK, FEATURES)
    phi_k = head_features(key_rows, projector).reshape(blocks, BLOCK, FEATURES)
    value_blocks = values.reshape(blocks, BLOCK, HEAD_DIM)
    row_index = lax.broadcasted_iota(jnp.int32, (BLOCK, BLOCK), 0)
    col_index = lax.broadcasted_iota(jnp.int32, (BLOCK, BLOCK), 1)
    causal = col_index <= row_index

    def step(running, pieces):
        memory, key_sum = running
        block_q, block_k, block_v = pieces
        scores = low_back(low(jnp.where(causal, jnp.dot(block_q, block_k.T, precision=HIGH), 0.0)))
        numerator = low_back(jnp.dot(scores, block_v, precision=HIGH) + jnp.dot(block_q, low(memory), precision=HIGH))
        denominator = lax.optimization_barrier(jnp.sum(scores, axis=-1)) + jnp.dot(block_q, low(key_sum), precision=HIGH)
        memory = memory + low_back(jnp.dot(block_k.T, block_v, precision=HIGH))
        key_sum = key_sum + lax.optimization_barrier(jnp.sum(block_k, axis=0))
        return ((memory, key_sum), numerator / denominator[:, None])
    start_state = (jnp.zeros((FEATURES, HEAD_DIM), jnp.float32), jnp.zeros((FEATURES,), jnp.float32))
    _, outputs = lax.scan(jax.checkpoint(step), start_state, (phi_q, phi_k, value_blocks))
    return outputs.reshape(length, HEAD_DIM)

def forward(inputs, proj_qkv, proj_out, proj_up, proj_down, norm_g, norm_b, projector):
    length = inputs.shape[0]
    normed = low(normalize(inputs, norm_g[0], norm_b[0]))
    mixed_qkv = low_back(low(jnp.einsum('ld,dce->lce', normed, proj_qkv, precision=HIGH)))
    shaped = mixed_qkv.reshape(length, 3, HEADS, HEAD_DIM).transpose(1, 2, 0, 3)
    attended = jax.vmap(head_attention)(shaped[0], shaped[1], shaped[2], projector)
    joined = low(attended.transpose(1, 0, 2).reshape(length, D))
    residual = inputs + low_back(jnp.dot(joined, proj_out, precision=HIGH))
    second_normed = low(normalize(residual, norm_g[1], norm_b[1]))
    pre_act = low_back(jnp.dot(second_normed, proj_up, precision=HIGH))
    activated = low(jax.nn.gelu(pre_act, approximate=False))
    return residual + low_back(jnp.dot(activated, proj_down, precision=HIGH))

def reference(tokens, cotangent, w_qkv, w_out, w_up, w_down, gains, shifts, feat_fresh, feat_last, flags):
    projector = jnp.where((flags == 1)[:, None, None], feat_fresh.astype(jnp.float32)[None], feat_last.astype(jnp.float32)[None])
    weights = (w_qkv.astype(jnp.float32), w_out.astype(jnp.float32), w_up.astype(jnp.float32), w_down.astype(jnp.float32), gains.astype(jnp.float32), shifts.astype(jnp.float32))
    sequences = tokens.astype(jnp.float32).reshape(SEQS, SEQ_LEN, D)
    cot_rows = cotangent.astype(jnp.float32).reshape(SEQS, SEQ_LEN, D)

    def apply(inputs, proj_qkv, proj_out, proj_up, proj_down, norm_g, norm_b):
        return forward(inputs, proj_qkv, proj_out, proj_up, proj_down, norm_g, norm_b, projector)

    def run(sums, pair):
        sequence, cot_seq = pair
        result, pull = jax.vjp(apply, sequence, weights[0], weights[1], weights[2], weights[3], weights[4], weights[5])
        grads = pull(cot_seq)
        new_sums = tuple((before + adding for before, adding in zip(sums, grads[1:])))
        return (new_sums, (result, grads[0]))
    zero_sums = tuple((jnp.zeros_like(weight) for weight in weights))
    sums, (results, grad_rows) = lax.scan(run, zero_sums, (sequences, cot_rows))
    return (results.reshape(TOKENS, D), grad_rows.reshape(TOKENS, D), sums[0], sums[1], sums[2], sums[3], sums[4], sums[5])
```

```python
import jax
import jax.numpy as jnp
from jax import lax
from jax.sharding import PartitionSpec as P

HEAD_DIM = 64
FEATURES = 256
EPS = 1e-05
F32 = jnp.float32
BF16 = jnp.bfloat16


def normalize(inputs, norm_gain, offset):
    average = jnp.mean(inputs, axis=-1, keepdims=True)
    centered = inputs - average
    variance = jnp.mean(centered * centered, axis=-1, keepdims=True)
    return centered * lax.rsqrt(variance + EPS) * norm_gain + offset


def gelu_exact(inputs):
    return jax.nn.gelu(inputs, approximate=False)


def mul(spec, *operands):
    return jnp.einsum(spec, *operands, preferred_element_type=F32)


def split_heads(matrix):
    length = matrix.shape[0]
    return jnp.transpose(matrix.reshape(length, -1, HEAD_DIM), (1, 0, 2))


def join_heads(stacked):
    moved = jnp.transpose(stacked, (1, 0, 2))
    return moved.reshape(moved.shape[0], -1)


def features(inputs, projector):
    factor = HEAD_DIM ** (-0.25)
    projected = mul("hlc,hcm->hlm", inputs, projector)
    wide_in = inputs.astype(F32)
    squares = 0.5 * factor * factor * jnp.sum(wide_in * wide_in, axis=-1, keepdims=True)
    return jnp.exp(factor * projected - squares) * FEATURES ** (-0.5)


def features_back(inputs, projector, expo, grad_phi):
    factor = HEAD_DIM ** (-0.25)
    grad_pre = grad_phi * expo
    grad_proj = (factor * grad_pre).astype(BF16)
    through = mul("hlm,hcm->hlc", grad_proj, projector)
    return through - factor * factor * jnp.sum(grad_pre, axis=-1, keepdims=True) * inputs.astype(F32)


def from_others(part, before):
    parts = lax.all_gather(part, "tensor")
    mine = lax.axis_index("tensor")
    place = jnp.arange(parts.shape[0])
    taken = (place < mine) if before else (place > mine)
    return jnp.sum(jnp.where(taken[:, None, None, None], parts, 0.0), axis=0)


def with_sums(values):
    return jnp.concatenate([values, jnp.ones_like(values[..., :1])], axis=-1)


def plain(
    tokens, cotangent, w_qkv, w_out, w_up, w_down, gains, shifts, feat_fresh, feat_last, flags
):
    w_qkv = lax.all_gather(w_qkv, "tensor", axis=2, tiled=True)
    w_out = lax.all_gather(w_out, "tensor", axis=0, tiled=True)
    w_up = lax.all_gather(w_up, "tensor", axis=1, tiled=True)
    w_down = lax.all_gather(w_down, "tensor", axis=0, tiled=True)
    inputs = tokens.astype(F32)
    rows = inputs.shape[0]
    normed, first_pull = jax.vjp(normalize, inputs, gains[0], shifts[0])
    normed = normed.astype(BF16)
    projector = jnp.where((flags == 1)[:, None, None], feat_fresh[None], feat_last[None])
    mixed = mul("ld,dce->cle", normed, w_qkv).astype(BF16)
    queries, keys, values = (split_heads(mixed[c]) for c in range(3))
    expo_q, expo_k = features(queries, projector), features(keys, projector)
    phi_q, phi_k = expo_q.astype(BF16), expo_k.astype(BF16)
    summed_values = with_sums(values)
    memory = from_others(mul("hkm,hke->hme", phi_k, summed_values), True).astype(BF16)
    causal = jnp.tril(jnp.ones((rows, rows), jnp.bool_))
    scores = jnp.where(causal, mul("hcm,hkm->hck", phi_q, phi_k), 0.0).astype(BF16)
    both = mul("hck,hke->hce", scores, summed_values) + mul("hcm,hme->hce", phi_q, memory)
    denoms = both[..., -1:]
    outputs = both[..., :-1] / denoms
    joined = join_heads(outputs).astype(BF16)
    residual = inputs + mul("le,ed->ld", joined, w_out)
    second, second_pull = jax.vjp(normalize, residual, gains[1], shifts[1])
    second = second.astype(BF16)
    pre_act = mul("ld,df->lf", second, w_up)
    activated, gelu_pull = jax.vjp(gelu_exact, pre_act)
    act_low = activated.astype(BF16)
    result = residual + mul("lf,fd->ld", act_low, w_down)
    grad_act = mul("ld,fd->lf", cotangent, w_down)
    grad_pre = gelu_pull(grad_act)[0].astype(BF16)
    grad_down = mul("ld,lf->df", cotangent, act_low)
    grad_up = mul("ld,lf->df", second, grad_pre)
    grad_resid, grad_gain2, grad_shift2 = second_pull(mul("lf,df->ld", grad_pre, w_up))
    grad_resid = grad_resid + cotangent.astype(F32)
    resid_low = grad_resid.astype(BF16)
    grad_out = split_heads(mul("ld,ed->le", resid_low, w_out))
    grad_wout = mul("ld,le->de", resid_low, joined)
    grad_num = (grad_out / denoms).astype(BF16)
    grad_den = -jnp.sum(grad_out * outputs, axis=-1, keepdims=True) / denoms
    grad_both = jnp.concatenate([grad_num, grad_den.astype(BF16)], axis=-1)
    grad_memory = from_others(mul("hcm,hce->hme", phi_q, grad_both), False).astype(BF16)
    grad_scores = jnp.where(
        causal, (mul("hce,hke->hck", grad_num, values) + grad_den).astype(BF16), 0
    )
    grad_q = mul("hck,hkm->hcm", grad_scores, phi_k) + mul("hce,hme->hcm", grad_both, memory)
    grad_k = mul("hck,hcm->hkm", grad_scores, phi_q)
    grad_k = grad_k + mul("hke,hme->hkm", summed_values, grad_memory)
    grad_v = mul("hck,hce->hke", scores, grad_num)
    grad_v = grad_v + mul("hkm,hme->hke", phi_k, grad_memory[..., :-1])
    grad_mixed = jnp.stack(
        [
            join_heads(features_back(queries, projector, expo_q, grad_q)),
            join_heads(features_back(keys, projector, expo_k, grad_k)),
            join_heads(grad_v),
        ]
    ).astype(BF16)
    grad_wqkv = mul("ld,cle->dce", normed, grad_mixed)
    grad_normed = mul("cle,dce->ld", grad_mixed, w_qkv)
    grad_inputs, grad_gain1, grad_shift1 = first_pull(grad_normed)
    grad_tokens = grad_resid + grad_inputs

    tensor, dp = lax.axis_size("tensor"), lax.axis_size("dp")
    wide = grad_wqkv.shape[0]

    def by_owner(grad):
        shaped = grad.reshape(dp, wide // dp, -1, tensor, grad.shape[-1] // tensor)
        moved = jnp.transpose(shaped, (0, 3, 1, 2, 4))
        return moved.reshape(dp * tensor, wide // dp, -1).astype(BF16)

    packed = jnp.concatenate(
        [by_owner(g) for g in (grad_wqkv, grad_wout, grad_up, grad_down)], axis=2
    )
    owned = lax.psum_scatter(packed, ("dp", "tensor"), scatter_dimension=0, tiled=True)[0]
    owned = owned.astype(F32)
    edge = [3 * wide // tensor, 4 * wide // tensor, 4 * wide // tensor + w_up.shape[1] // tensor]
    own_qkv, own_wout, own_up, own_down = jnp.split(owned, edge, axis=1)
    grad_gains, grad_shifts = lax.psum(
        (jnp.stack([grad_gain1, grad_gain2]), jnp.stack([grad_shift1, grad_shift2])),
        ("dp", "tensor"),
    )
    return (
        result,
        grad_tokens,
        own_qkv.reshape(wide // dp, 3, wide // tensor),
        own_wout.T,
        own_up,
        own_down.T,
        grad_gains,
        grad_shifts,
    )


def solution(mesh):
    placed = (
        P(("dp", "tensor"), None),
        P(("dp", "tensor"), None),
        P(None, None, "tensor"),
        P("tensor", None),
        P(None, "tensor"),
        P("tensor", None),
        P(),
        P(),
        P(),
        P(),
        P(),
    )
    return jax.shard_map(
        plain,
        mesh=mesh,
        in_specs=placed,
        out_specs=(
            P(("dp", "tensor"), None),
            P(("dp", "tensor"), None),
            P("dp", None, "tensor"),
            P("tensor", "dp"),
            P("dp", "tensor"),
            P("tensor", "dp"),
            P(),
            P(),
        ),
        check_vma=False,
    )
```

```python
import jax
import jax.numpy as jnp
from jax import lax
from jax.experimental import pallas as pl
from jax.experimental.pallas import tpu as pltpu
from jax.sharding import PartitionSpec as P

HEAD_DIM = 64
FEATURES = 256
EPS = 1e-05
F32 = jnp.float32
BF16 = jnp.bfloat16
FACTOR = HEAD_DIM ** (-0.25)
ROWS, WIDE, TILE, FF = 1024, 512, 256, 2048
TILES = ROWS // TILE
PAIRS = 4


def nn(a, b):
    return lax.dot_general(a, b, (((1,), (0,)), ((), ())), preferred_element_type=F32)


def nt(a, b):
    return lax.dot_general(a, b, (((1,), (1,)), ((), ())), preferred_element_type=F32)


def tn(a, b):
    return lax.dot_general(a, b, (((0,), (0,)), ((), ())), preferred_element_type=F32)


def iota(shape, dim):
    return lax.broadcasted_iota(jnp.int32, shape, dim)


def row_tile(t):
    return pl.ds(pl.multiple_of(t * TILE, TILE), TILE)


def lane_tile(j, width=128):
    return pl.ds(pl.multiple_of(j * width, width), width)


def loop(n, body):
    lax.fori_loop(0, n, lambda i, c: (body(i), c)[1], 0)


def of_head(shape, dim, head):
    return (iota(shape, dim) & HEAD_DIM) == head * HEAD_DIM


def centre(v):
    mean = jnp.mean(v, axis=-1, keepdims=True)
    off = v - mean
    rstd = lax.rsqrt(jnp.mean(off * off, axis=-1, keepdims=True) + EPS)
    return off * rstd, rstd


def centre_back(grad, hat, rstd, gain):
    scaled = grad * gain
    first = jnp.mean(scaled, axis=-1, keepdims=True)
    second = jnp.mean(scaled * hat, axis=-1, keepdims=True)
    return rstd * (scaled - first - hat * second)


def gelu_and_slope(u):
    bell = jnp.exp(-0.5 * u * u)
    t = 1.0 / (1.0 + (0.3275911 * 0.7071067811865476) * jnp.abs(u))
    poly = 0.5 * 1.061405429
    for c in (-1.453152027, 1.421413741, -0.284496736, 0.254829592):
        poly = poly * t + 0.5 * c
    tail = poly * t * bell
    cdf = jnp.where(u >= 0, 1.0 - tail, tail)
    return u * cdf, cdf + (0.3989422804014327 * u) * bell


def features_of(rows, wf):
    wide = rows.astype(F32)
    both = jnp.concatenate([rows, ((0.5 * FACTOR) * wide * wide).astype(BF16)], axis=1)
    return (jnp.exp(FACTOR * nn(both, wf)) * FEATURES ** (-0.5)).astype(BF16)


def features_back(rows, wf, weighted):
    through = nt(weighted, wf)
    half = 2 * HEAD_DIM
    return FACTOR * through[:, :half] + (FACTOR * FACTOR) * through[:, half:] * rows.astype(F32)


def merge_heads(state):
    own = of_head((state.shape[0], FEATURES), 0, 0)
    return jnp.where(own, state[:, :FEATURES], state[:, FEATURES:])


class Phases:
    def __init__(self, **refs):
        self.__dict__.update(refs)

    def set_up(self):
        self.vx[:, :, 128:] = jnp.ones((PAIRS, ROWS, 128), BF16)
        fresh, last = self.fresh[...], self.last[...]
        zero = jnp.zeros((HEAD_DIM, FEATURES), BF16)
        minus = jnp.full((HEAD_DIM, FEATURES), -1.0, BF16)
        for j in range(PAIRS):
            for head in range(2):
                flag = (self.flags[2 * j + head] == 1).astype(F32)
                omega = (flag * fresh.astype(F32) + (1.0 - flag) * last.astype(F32)).astype(BF16)
                for lower, block in ((0, omega), (128, minus)):
                    for other in range(2):
                        at = pl.ds(lower + head * HEAD_DIM, HEAD_DIM)
                        col = pl.ds(other * FEATURES, FEATURES)
                        self.wf[j, at, col] = block if other == head else zero
        self.small[...] = jnp.zeros(self.small.shape, F32)

    def norm1(self):
        def body(t):
            hat, _ = centre(self.tokens[row_tile(t), :].astype(F32))
            self.n1[row_tile(t), :] = (hat * self.gains[0:1, :] + self.shifts[0:1, :]).astype(BF16)

        loop(TILES, body)

    def project(self, hh):
        for jj in range(2):
            self.run[jj] = jnp.zeros((TILE, FEATURES), F32)

        def body(t):
            rows = self.n1[row_tile(t), :]
            parts = [
                nn(rows, self.wqkv[hh, :, c * 256 : (c + 1) * 256]).astype(BF16) for c in range(3)
            ]
            for jj in range(2):
                j = 2 * hh + jj
                q, k, v = (p[:, jj * 128 : (jj + 1) * 128] for p in parts)
                self.q[j, row_tile(t), :] = q
                self.k[j, row_tile(t), :] = k
                self.vx[j, row_tile(t), 0:128] = v
                wf = self.wf[j]
                self.phi_q[j, row_tile(t), :] = features_of(q, wf)
                phi_k = features_of(k, wf)
                self.phi_k[j, row_tile(t), :] = phi_k
                state = merge_heads(tn(self.vx[j, row_tile(t), :], phi_k))
                self.zt[j * TILES + t] = state.astype(BF16)
                self.run[jj] += state

        loop(TILES, body)
        for jj in range(2):
            self.pack(self.zsend, 2 * hh + jj, self.run.at[jj], False)

    def pack(self, out, j, state, gradient):
        first, second = state[128:136, :], state[192:200, :]
        if gradient:
            first = 0.5 * (first + state[160:168, :])
            second = 0.5 * (second + state[224:232, :])
        out[j, 0:128, :] = state[0:128, :].astype(BF16)
        out[j, 128:136, :] = first.astype(BF16)
        out[j, 136:144, :] = second.astype(BF16)

    def unpack(self, packed):
        low = packed.astype(F32)
        sums = [jnp.broadcast_to(low[r : r + 1], (HEAD_DIM, FEATURES)) for r in (128, 136)]
        return jnp.concatenate([low[0:128], *sums], axis=0)

    def attend(self, hh, start):
        for jj in range(2):
            j = 2 * hh + jj
            self.run[0] = start(j)

            def body(t, j=j):
                at = row_tile(t)
                before = self.run[0]
                low = before.astype(BF16)
                self.run[0] = before + self.zt[j * TILES + t].astype(F32)
                self.zt[j * TILES + t] = low
                vx = self.vx[j, at, :]
                both = []
                for head in range(2):
                    f = slice(head * FEATURES, (head + 1) * FEATURES)
                    phi_q, phi_k = self.phi_q[j, at, f], self.phi_k[j, at, f]
                    s = nt(phi_q, phi_k)
                    s = jnp.where(iota(s.shape, 1) <= iota(s.shape, 0), s, 0.0).astype(BF16)
                    both.append(nn(s, vx) + nt(phi_q, low))
                r = jnp.where(of_head(both[0].shape, 1, 0), both[0], both[1])
                inverse = 1.0 / r[:, 128:]
                self.a[at, lane_tile(j)] = (r[:, :128] * inverse).astype(BF16)
                self.inverse[j, at, :] = inverse

            loop(TILES, body)

    def norm2(self):
        def body(t):
            at = row_tile(t)
            w_out = self.wout[...].reshape(WIDE, WIDE)
            h = self.tokens[at, :].astype(F32) + nn(self.a[at, :], w_out)
            self.out[at, :] = h
            hat, rstd = centre(h)
            self.hat2[at, :] = hat.astype(BF16)
            self.rstd2[at, :] = jnp.broadcast_to(rstd, (TILE, 128))
            self.n2[at, :] = (hat * self.gains[1:2, :] + self.shifts[1:2, :]).astype(BF16)
            self.grad[at, :] = jnp.zeros((TILE, WIDE), F32)

        loop(TILES, body)

    def feed(self, slot):
        def body(i):
            t, p = lax.div(i, 2), lax.rem(i, 2)
            at, cols = row_tile(t), lane_tile(p, 512)
            w_up, w_down = self.wup[slot, :, cols], self.wdown[slot, cols, :]
            g, slope = gelu_and_slope(nn(self.n2[at, :], w_up))
            g = g.astype(BF16)
            du = (slope * nt(self.cot[at, :], w_down)).astype(BF16)
            self.g[t * 4 + slot * 2 + p] = g
            self.du[t * 4 + slot * 2 + p] = du
            self.out[at, :] += nn(g, w_down)
            self.grad[at, :] += nt(du, w_up)

        loop(2 * TILES, body)

    def norm2_back(self):
        def body(t):
            at = row_tile(t)
            grad, hat = self.grad[at, :], self.hat2[at, :].astype(F32)
            self.small[1:2, :] += jnp.sum(grad * hat, axis=0, keepdims=True)
            self.small[3:4, :] += jnp.sum(grad, axis=0, keepdims=True)
            back = centre_back(grad, hat, self.rstd2[at, 0:1], self.gains[1:2, :])
            dh = self.cot[at, :].astype(F32) + back
            self.grad[at, :] = dh
            self.dhb[at, :] = dh.astype(BF16)

        loop(TILES, body)

    def flip(self, source, out):
        def body(t):
            out[:, row_tile(t)] = source[row_tile(t), :].T

        loop(TILES, body)

    def weight_grad(self, xt, blocks, n_cols, store):
        def body(c):
            total = nn(xt[:, 0:TILE], blocks(0, c))
            for t in range(1, TILES):
                total = total + nn(xt[:, t * TILE : (t + 1) * TILE], blocks(t, c))
            store(c, total)

        loop(n_cols, body)

    def attend_back_start(self):
        def body(t):
            at = row_tile(t)
            w_out = self.wout[...].reshape(WIDE, WIDE)
            da = nt(self.dhb[at, :], w_out)
            o = self.a[at, :].astype(F32)
            same = (iota((128, 128), 0) & HEAD_DIM) == (iota((128, 128), 1) & HEAD_DIM)
            ones = jnp.where(same, 1.0, 0.0).astype(BF16)
            high = (iota((TILE, 128), 1) & 32) == 0
            for j in range(PAIRS):
                lanes = slice(j * 128, (j + 1) * 128)
                do, inverse = da[:, lanes], self.inverse[j, at, :]
                dden = -nn((do * o[:, lanes]).astype(BF16), ones) * inverse
                top = dden.astype(BF16)
                rest = (dden - top.astype(F32)).astype(BF16)
                self.dnx[j, at, 0:128] = (do * inverse).astype(BF16)
                self.dnx[j, at, 128:] = jnp.where(high, top, rest) * jnp.asarray(1 / 32, BF16)

        loop(TILES, body)

    def sums_back(self, j):
        self.run[0] = jnp.zeros((TILE, FEATURES), F32)

        def body(t):
            at = row_tile(t)
            state = merge_heads(tn(self.dnx[j, at, :], self.phi_q[j, at, :]))
            self.gt[j * TILES + t] = state.astype(BF16)
            self.run[0] += state

        loop(TILES, body)
        self.pack(self.gsend, j, self.run.at[0], True)

    def back_q(self, j):
        def body(t):
            at = row_tile(t)
            dnx = self.dnx[j, at, :]
            w = []
            for head in range(2):
                f = slice(head * FEATURES, (head + 1) * FEATURES)
                own = jnp.where(of_head(dnx.shape, 1, head), dnx, jnp.zeros_like(dnx))
                ds = nt(own, self.vx[j, at, :])
                ds = jnp.where(iota(ds.shape, 1) <= iota(ds.shape, 0), ds, 0.0).astype(BF16)
                dphi = nn(ds, self.phi_k[j, at, f]) + nn(own, self.zt[j * TILES + t])
                w.append((dphi * self.phi_q[j, at, f].astype(F32)).astype(BF16))
            dq = features_back(self.q[j, at, :], self.wf[j], jnp.concatenate(w, axis=1))
            self.dqkv[0 * TILES + t, :, lane_tile(j)] = dq.astype(BF16)

        loop(TILES, body)

    def back_kv(self, j, start):
        self.run[0] = start(j)

        def body(i):
            t = TILES - 1 - i
            at = row_tile(t)
            after = self.run[0]
            low = after.astype(BF16)
            self.run[0] = after + self.gt[j * TILES + t].astype(F32)
            dnx, vx = self.dnx[j, at, :], self.vx[j, at, :]
            w, dv = [], []
            for head in range(2):
                f = slice(head * FEATURES, (head + 1) * FEATURES)
                phi_q, phi_k = self.phi_q[j, at, f], self.phi_k[j, at, f]
                st = nt(phi_k, phi_q)
                upper = iota(st.shape, 0) <= iota(st.shape, 1)
                st = jnp.where(upper, st, 0.0).astype(BF16)
                own = jnp.where(of_head(vx.shape, 1, head), vx, jnp.zeros_like(vx))
                dst = nt(own, dnx)
                dst = jnp.where(upper, dst, 0.0).astype(BF16)
                dphi = nn(dst, phi_q) + nn(own, low)
                w.append((dphi * phi_k.astype(F32)).astype(BF16))
                dv.append(nn(st, dnx[:, 0:128]) + nt(phi_k, low[0:128]))
            dk = features_back(self.k[j, at, :], self.wf[j], jnp.concatenate(w, axis=1))
            self.dqkv[1 * TILES + t, :, lane_tile(j)] = dk.astype(BF16)
            dv = jnp.where(of_head(dv[0].shape, 1, 0), dv[0], dv[1])
            self.dqkv[2 * TILES + t, :, lane_tile(j)] = dv.astype(BF16)

        loop(TILES, body)

    def norm1_back(self):
        def body(t):
            at = row_tile(t)
            grad = jnp.zeros((TILE, WIDE), F32)
            for hh in range(2):
                for c in range(3):
                    part = self.dqkv[c * TILES + t, :, hh * 256 : (hh + 1) * 256]
                    grad = grad + nt(part, self.wqkv[hh, :, c * 256 : (c + 1) * 256])
            hat, rstd = centre(self.tokens[at, :].astype(F32))
            self.small[0:1, :] += jnp.sum(grad * hat, axis=0, keepdims=True)
            self.small[2:3, :] += jnp.sum(grad, axis=0, keepdims=True)
            self.grad[at, :] += centre_back(grad, hat, rstd, self.gains[0:1, :])

        loop(TILES, body)


def work_buffers():
    vmem = pltpu.VMEM
    return dict(
        n1=vmem((ROWS, WIDE), BF16),
        q=vmem((PAIRS, ROWS, 128), BF16),
        k=vmem((PAIRS, ROWS, 128), BF16),
        vx=vmem((PAIRS, ROWS, 256), BF16),
        phi_q=vmem((PAIRS, ROWS, 512), BF16),
        phi_k=vmem((PAIRS, ROWS, 512), BF16),
        zt=vmem((PAIRS * TILES, 256, 256), BF16),
        gt=vmem((PAIRS * TILES, 256, 256), BF16),
        run=vmem((2, 256, 256), F32),
        wf=vmem((PAIRS, 256, 512), BF16),
        a=vmem((ROWS, WIDE), BF16),
        inverse=vmem((PAIRS, ROWS, 128), F32),
        n2=vmem((ROWS, WIDE), BF16),
        hat2=vmem((ROWS, WIDE), BF16),
        rstd2=vmem((ROWS, 128), F32),
        g=vmem((TILES * 4, 256, 512), BF16),
        du=vmem((TILES * 4, 256, 512), BF16),
        dhb=vmem((ROWS, WIDE), BF16),
        dnx=vmem((PAIRS, ROWS, 256), BF16),
        zsend=vmem((PAIRS, 144, 256), BF16),
        gsend=vmem((PAIRS, 144, 256), BF16),
        xt=vmem((WIDE, ROWS), BF16),
        xt2=vmem((WIDE, ROWS), BF16),
        small=vmem((4, WIDE), F32),
    )


MESH = pl.DeviceIdType.MESH
OWNED = 1024


class Links:
    def __init__(self, deep, refs):
        self.deep = deep
        self.__dict__.update(refs)
        self.dp, self.me = lax.axis_index("dp"), lax.axis_index("tensor")
        self.core = lax.rem(self.dp, 2)
        self.x = lax.rem(lax.div(self.dp, 2), 2)
        self.z = lax.div(self.dp, 4)
        self.block = WIDE // (4 * deep)

    def place(self, axis, step=1):
        dp, me = self.dp, self.me
        if axis == "core":
            return dict(dp=dp + 1 - 2 * self.core, tensor=me)
        if axis == "x":
            return dict(dp=dp + 2 - 4 * self.x, tensor=me)
        if axis == "y":
            return dict(dp=dp, tensor=1 - me)
        return dict(dp=dp + 4 * (lax.rem(self.z + step, self.deep) - self.z), tensor=me)

    def partners(self):
        steps = [self.place("z", s) for s in range(1, self.deep)]
        return [self.place(a) for a in ("core", "x", "y")] + steps

    def greet(self):
        barrier = pltpu.get_barrier_semaphore()
        for where in self.partners():
            pl.semaphore_signal(barrier, inc=1, device_id=where, device_id_type=MESH)

    def met(self):
        pl.semaphore_wait(pltpu.get_barrier_semaphore(), len(self.partners()))

    def copy(self, source, target, sems, at, where):
        return pltpu.make_async_remote_copy(
            src_ref=source,
            dst_ref=target,
            send_sem=sems.at[2 * at],
            recv_sem=sems.at[2 * at + 1],
            device_id=where,
            device_id_type=MESH,
        )


    def weight(self, i):
        source = (self.wqkv_in, self.wout_in, self.wup_in, self.wdown_in)[i]
        return source, (self.wqkv, self.wout, self.wup, self.wdown)[i], source.shape[0] // 2

    def own_weight(self, i):
        source, slots, _ = self.weight(i)
        return pltpu.make_async_copy(source, slots.at[self.me], self.own_sems.at[i])

    def weight_over(self, i):
        source, slots, half = self.weight(i)
        part = pl.ds(pl.multiple_of(self.core * half, half), half)
        target = slots.at[self.me, part]
        return self.copy(source.at[part], target, self.over_sems, i, self.place("y"))

    def weight_along(self, i):
        _, slots, half = self.weight(i)
        part = pl.ds(pl.multiple_of(self.core * half, half), half)
        held = slots.at[1 - self.me, part]
        return self.copy(held, held, self.along_sems, i, self.place("core"))


    def axes(self, seg):
        return ("y", "x") if seg != 1 else ("x", "y")

    def index(self, axis):
        return self.me if axis == "y" else self.x

    def stage(self, seg, depth):
        grads = self.grads[seg]
        if depth == 0:
            source = grads.at[1 - self.core]
            return self.copy(source, self.got[seg][0], self.sum_sems[seg], 0, self.place("core"))
        axis = self.axes(seg)[depth - 1]
        start, size = self.span(seg, depth, 1 - self.index(axis))
        source = grads.at[self.core, pl.ds(pl.multiple_of(start, self.block), size)]
        return self.copy(source, self.got[seg][depth], self.sum_sems[seg], depth, self.place(axis))

    def span(self, seg, depth, last):
        start, size = 0, WIDE
        for i in range(depth):
            size = size // 2
            at = last if i == depth - 1 else self.index(self.axes(seg)[i])
            start = start + at * size
        return start, size

    def mine(self, seg, depth):
        if depth == 0:
            return 0, WIDE
        return self.span(seg, depth, self.index(self.axes(seg)[depth - 1]))

    def start(self, seg, depth):
        self.stage(seg, depth).start()

    def finish(self, seg, depth):
        self.stage(seg, depth).wait()
        start, size = self.mine(seg, depth)
        grads, got = self.grads[seg], self.got[seg][depth]
        step = min(size, 64)

        def body(i):
            there = pl.ds(pl.multiple_of(i * step, step), step)
            here = pl.ds(pl.multiple_of(start + i * step, step), step)
            grads[self.core, here] = grads[self.core, here] + got[there]

        loop(size // step, body)

    def z_copy(self, seg, step):
        start, _ = self.mine(seg, 2)
        row = start + lax.rem(self.z + step, self.deep) * self.block
        source = self.grads[seg].at[self.core, pl.ds(pl.multiple_of(row, self.block), self.block)]
        target = self.got[seg][3].at[step - 1]
        return self.copy(source, target, self.sum_sems[seg], 2 + step, self.place("z", step))

    def start_z(self, seg):
        for step in range(1, self.deep):
            self.z_copy(seg, step).start()

    def finish_z(self, seg, out):
        start, _ = self.mine(seg, 2)
        here = pl.ds(pl.multiple_of(start + self.z * self.block, self.block), self.block)
        total = self.grads[seg][self.core, here].astype(F32)
        for step in range(1, self.deep):
            self.z_copy(seg, step).wait()
            total = total + self.got[seg][3][step - 1].astype(F32)
        out[...] = total


    def small_sum(self, small, heard):
        slot = 0
        for axis in ("core", "y", "x"):
            both = self.copy(small, heard.at[slot], self.small_sems, slot, self.place(axis))
            both.start()
            both.wait()
            small[...] = small[...] + heard[slot]
            slot += 1
        copies = [
            self.copy(small, heard.at[2 + s], self.small_sems, 2 + s, self.place("z", s))
            for s in range(1, self.deep)
        ]
        for both in copies:
            both.start()
        for both in copies:
            both.wait()
        total = small[...]
        for s in range(1, self.deep):
            total = total + heard[2 + s]
        return total


def scatter(grads, deep, c_of):
    block = WIDE // (4 * deep)

    def store(c, total):
        tensor, col = c_of(c)
        low = total.astype(BF16)
        for d in range(4 * deep):
            core, x, z = d % 2, d // 2 % 2, d // 4
            ref, flipped = grads
            near, far = (x, tensor) if flipped else (tensor, x)
            row = ((near * 2 + far) * deep + z) * block
            here = pl.ds(pl.multiple_of(row, block), block)
            ref[core, here, lane_tile(col, TILE)] = low[d * block : (d + 1) * block]

    return store


def layer_kernel(deep, names, *refs):
    r = dict(zip(names, refs))
    sends = r["sum_sems"]
    links = Links(
        deep,
        dict(
            r,
            grads=(r["grads0"], r["grads1"], r["wup"]),
            got=tuple(tuple(r[f"got{d}"].at[s] for d in range(4)) for s in range(3)),
            sum_sems=tuple(sends.at[s] for s in range(3)),
        ),
    )
    p = Phases(**r, dqkv=r["du"])
    me = links.me
    other = 1 - me

    links.greet()
    for i in range(4):
        links.own_weight(i).start()
    p.set_up()
    links.met()
    for i in range(2):
        links.weight_over(i).start()
    p.norm1()
    links.own_weight(0).wait()
    p.project(me)

    def pairs_of(ref, hh):
        return ref.at[pl.ds(2 * hh, 2)]

    def sums_to(source, target, sems, at, hh):
        return links.copy(pairs_of(source, hh), pairs_of(target, hh), sems, at, links.place("y"))

    @pl.when(me == 0)
    def _():
        p.zgot[...] = jnp.zeros(p.zgot.shape, BF16)
        sums_to(p.zsend, p.zgot, r["z_sems"], 0, 0).start()

    @pl.when(me == 1)
    def _():
        p.ggot[...] = jnp.zeros(p.ggot.shape, BF16)

    for i in range(2):
        links.weight_over(i).wait()
        links.weight_along(i).start()
    links.weight_along(0).wait()
    p.project(other)

    @pl.when(me == 0)
    def _():
        sums_to(p.zsend, p.zgot, r["z_sems"], 1, 1).start()

    for i in range(2, 4):
        links.weight_over(i).start()

    @pl.when(me == 1)
    def _():
        for hh in range(2):
            sums_to(p.zsend, p.zgot, r["z_sems"], hh, hh).wait_recv()

    for hh in (me, other):
        p.attend(hh, lambda j: p.unpack(p.zgot[j]))

    @pl.when(me == 0)
    def _():
        for hh in range(2):
            sums_to(p.zsend, p.zgot, r["z_sems"], hh, hh).wait_send()

    links.own_weight(1).wait()
    links.weight_along(1).wait()
    p.norm2()
    links.own_weight(2).wait()
    links.own_weight(3).wait()
    p.feed(me)
    for i in range(2, 4):
        links.weight_over(i).wait()
        links.weight_along(i).start()
    for i in range(2, 4):
        links.weight_along(i).wait()
    p.feed(other)

    p.norm2_back()
    p.attend_back_start()
    loop(PAIRS, p.sums_back)

    def grad_sums():
        return links.copy(p.gsend, p.ggot, r["g_sems"], 0, links.place("y"))

    @pl.when(me == 1)
    def _():
        grad_sums().start()

    def by_ff(c):
        return lax.div(c, 4), lax.rem(c, 4)

    def half_block(ref):
        return lambda t, c: ref[t * 4 + lax.div(c, 2), :, lane_tile(lax.rem(c, 2), TILE)]

    p.flip(p.n2, p.xt)
    p.weight_grad(p.xt, half_block(p.du), 8, scatter((links.grads[0], False), deep, by_ff))
    links.start(0, 0)
    p.flip(p.cot, p.xt2)
    p.weight_grad(p.xt2, half_block(p.g), 8, scatter((links.grads[1], True), deep, by_ff))
    links.start(1, 0)
    links.finish(0, 0)
    links.start(0, 1)
    p.flip(p.dhb, p.xt)
    p.weight_grad(
        p.xt,
        lambda t, c: p.a[pl.ds(t * TILE, TILE), lane_tile(c, TILE)],
        2,
        scatter((links.grads[2], False), deep, lambda c: (c, 0)),
    )
    links.finish(1, 0)
    links.start(1, 1)
    return p, links, r


def layer_rest(deep, p, links, r):
    me = links.me
    loop(2, p.back_q)
    loop(2, lambda j: p.back_q(j + 2))
    for seg in range(2):
        links.finish(seg, 1)
        links.start(seg, 2)

    def grad_sums():
        return links.copy(p.gsend, p.ggot, r["g_sems"], 0, links.place("y"))

    @pl.when(me == 0)
    def _():
        grad_sums().wait_recv()

    @pl.when(me == 1)
    def _():
        grad_sums().wait_send()

    def back(j):
        p.back_kv(j, lambda j: p.unpack(p.ggot[j]))

    loop(2, back)
    for seg in range(2):
        links.finish(seg, 2)
        links.start_z(seg)
    loop(2, lambda j: back(j + 2))
    p.flip(p.n1, p.xt2)
    p.weight_grad(
        p.xt2,
        lambda t, c: p.dqkv[lax.div(c, 2) * TILES + t, :, lane_tile(lax.rem(c, 2), TILE)],
        6,
        scatter((links.grads[2], False), deep, lambda c: (lax.rem(c, 2), 1 + lax.div(c, 2))),
    )
    links.start(2, 0)
    p.norm1_back()
    links.finish(2, 0)
    links.start(2, 1)
    for seg in range(2):
        links.finish_z(seg, p.owned.at[seg])
    p.norms[...] = links.small_sum(p.small, p.heard)
    links.finish(2, 1)
    links.start(2, 2)
    links.finish(2, 2)
    links.start_z(2)
    links.finish_z(2, p.owned.at[2])


def layer_call(deep, tokens, cotangent, wqkv, wout, wup, wdown, gains, shifts, fresh, last, flags):
    vmem, hbm = pltpu.VMEM, pl.ANY
    block = WIDE // (4 * deep)
    inputs = dict(
        tokens=(tokens, vmem),
        cot=(cotangent, vmem),
        wqkv_in=(wqkv, hbm),
        wout_in=(wout, hbm),
        wup_in=(wup, hbm),
        wdown_in=(wdown, hbm),
        gains=(gains, vmem),
        shifts=(shifts, vmem),
        fresh=(fresh, vmem),
        last=(last, vmem),
        flags=(flags, pltpu.SMEM),
    )
    outputs = dict(
        out=jax.ShapeDtypeStruct((ROWS, WIDE), F32),
        grad=jax.ShapeDtypeStruct((ROWS, WIDE), F32),
        owned=jax.ShapeDtypeStruct((3, block, OWNED), F32),
        norms=jax.ShapeDtypeStruct((4, WIDE), F32),
    )
    dma = pltpu.SemaphoreType.DMA
    scratch = dict(
        work_buffers(),
        wqkv=vmem((2, WIDE, 768), BF16),
        wout=vmem((2, 256, WIDE), BF16),
        wup=vmem((2, WIDE, 1024), BF16),
        wdown=vmem((2, 1024, WIDE), BF16),
        zgot=vmem((PAIRS, 144, 256), BF16),
        ggot=vmem((PAIRS, 144, 256), BF16),
        grads0=vmem((2, WIDE, OWNED), BF16),
        grads1=vmem((2, WIDE, OWNED), BF16),
        got0=vmem((3, WIDE, OWNED), BF16),
        got1=vmem((3, WIDE // 2, OWNED), BF16),
        got2=vmem((3, WIDE // 4, OWNED), BF16),
        got3=vmem((3, deep - 1, block, OWNED), BF16),
        heard=vmem((2 + deep, 4, WIDE), F32),
        own_sems=dma((4,)),
        over_sems=dma((8,)),
        along_sems=dma((8,)),
        z_sems=dma((4,)),
        g_sems=dma((2,)),
        sum_sems=dma((3, 2 * (2 + deep))),
        small_sems=dma((2 * (2 + deep),)),
    )
    names = (*inputs, *outputs, *scratch)

    def kernel(*refs):
        layer_rest(deep, *layer_kernel(deep, names, *refs))

    return pl.pallas_call(
        kernel,
        out_shape=tuple(outputs.values()),
        in_specs=[pl.BlockSpec(memory_space=space) for _, space in inputs.values()],
        out_specs=tuple(pl.BlockSpec(memory_space=vmem) for _ in outputs),
        scratch_shapes=list(scratch.values()),
        compiler_params=pltpu.CompilerParams(
            collective_id=0, has_side_effects=True, vmem_limit_bytes=67043328
        ),
        name="layer",
    )(*(array for array, _ in inputs.values()))


def fused(
    tokens, cotangent, w_qkv, w_out, w_up, w_down, gains, shifts, feat_fresh, feat_last, flags
):
    deep = lax.axis_size("dp") // 4
    result, grad_tokens, owned, norms = layer_call(
        deep,
        tokens,
        cotangent,
        w_qkv.reshape(WIDE, 768),
        w_out,
        w_up,
        w_down,
        gains,
        shifts,
        feat_fresh,
        feat_last,
        flags,
    )
    rest = owned[2]
    return (
        result,
        grad_tokens,
        rest[:, 256:].reshape(-1, 3, 256),
        rest[:, :256].T,
        owned[0],
        owned[1].T,
        norms[:2],
        norms[2:],
    )


def fits(mesh):
    return mesh.shape["tensor"] == 2 and mesh.shape["dp"] % 4 == 0 and mesh.shape["dp"] <= 64


def normalize(inputs, norm_gain, offset):
    average = jnp.mean(inputs, axis=-1, keepdims=True)
    centered = inputs - average
    variance = jnp.mean(centered * centered, axis=-1, keepdims=True)
    return centered * lax.rsqrt(variance + EPS) * norm_gain + offset


def gelu_exact(inputs):
    return jax.nn.gelu(inputs, approximate=False)


def mul(spec, *operands):
    return jnp.einsum(spec, *operands, preferred_element_type=F32)


def split_heads(matrix):
    length = matrix.shape[0]
    return jnp.transpose(matrix.reshape(length, -1, HEAD_DIM), (1, 0, 2))


def join_heads(stacked):
    moved = jnp.transpose(stacked, (1, 0, 2))
    return moved.reshape(moved.shape[0], -1)


def plain_features(inputs, projector):
    factor = HEAD_DIM ** (-0.25)
    projected = mul("hlc,hcm->hlm", inputs, projector)
    wide_in = inputs.astype(F32)
    squares = 0.5 * factor * factor * jnp.sum(wide_in * wide_in, axis=-1, keepdims=True)
    return jnp.exp(factor * projected - squares) * FEATURES ** (-0.5)


def plain_features_back(inputs, projector, expo, grad_phi):
    factor = HEAD_DIM ** (-0.25)
    grad_pre = grad_phi * expo
    grad_proj = (factor * grad_pre).astype(BF16)
    through = mul("hlm,hcm->hlc", grad_proj, projector)
    return through - factor * factor * jnp.sum(grad_pre, axis=-1, keepdims=True) * inputs.astype(F32)


def from_others(part, before):
    parts = lax.all_gather(part, "tensor")
    mine = lax.axis_index("tensor")
    place = jnp.arange(parts.shape[0])
    taken = (place < mine) if before else (place > mine)
    return jnp.sum(jnp.where(taken[:, None, None, None], parts, 0.0), axis=0)


def with_sums(values):
    return jnp.concatenate([values, jnp.ones_like(values[..., :1])], axis=-1)


def plain(
    tokens, cotangent, w_qkv, w_out, w_up, w_down, gains, shifts, feat_fresh, feat_last, flags
):
    w_qkv = lax.all_gather(w_qkv, "tensor", axis=2, tiled=True)
    w_out = lax.all_gather(w_out, "tensor", axis=0, tiled=True)
    w_up = lax.all_gather(w_up, "tensor", axis=1, tiled=True)
    w_down = lax.all_gather(w_down, "tensor", axis=0, tiled=True)
    inputs = tokens.astype(F32)
    rows = inputs.shape[0]
    normed, first_pull = jax.vjp(normalize, inputs, gains[0], shifts[0])
    normed = normed.astype(BF16)
    projector = jnp.where((flags == 1)[:, None, None], feat_fresh[None], feat_last[None])
    mixed = mul("ld,dce->cle", normed, w_qkv).astype(BF16)
    queries, keys, values = (split_heads(mixed[c]) for c in range(3))
    expo_q, expo_k = plain_features(queries, projector), plain_features(keys, projector)
    phi_q, phi_k = expo_q.astype(BF16), expo_k.astype(BF16)
    summed_values = with_sums(values)
    memory = from_others(mul("hkm,hke->hme", phi_k, summed_values), True).astype(BF16)
    causal = jnp.tril(jnp.ones((rows, rows), jnp.bool_))
    scores = jnp.where(causal, mul("hcm,hkm->hck", phi_q, phi_k), 0.0).astype(BF16)
    both = mul("hck,hke->hce", scores, summed_values) + mul("hcm,hme->hce", phi_q, memory)
    denoms = both[..., -1:]
    outputs = both[..., :-1] / denoms
    joined = join_heads(outputs).astype(BF16)
    residual = inputs + mul("le,ed->ld", joined, w_out)
    second, second_pull = jax.vjp(normalize, residual, gains[1], shifts[1])
    second = second.astype(BF16)
    pre_act = mul("ld,df->lf", second, w_up)
    activated, gelu_pull = jax.vjp(gelu_exact, pre_act)
    act_low = activated.astype(BF16)
    result = residual + mul("lf,fd->ld", act_low, w_down)
    grad_act = mul("ld,fd->lf", cotangent, w_down)
    grad_pre = gelu_pull(grad_act)[0].astype(BF16)
    grad_down = mul("ld,lf->df", cotangent, act_low)
    grad_up = mul("ld,lf->df", second, grad_pre)
    grad_resid, grad_gain2, grad_shift2 = second_pull(mul("lf,df->ld", grad_pre, w_up))
    grad_resid = grad_resid + cotangent.astype(F32)
    resid_low = grad_resid.astype(BF16)
    grad_out = split_heads(mul("ld,ed->le", resid_low, w_out))
    grad_wout = mul("ld,le->de", resid_low, joined)
    grad_num = (grad_out / denoms).astype(BF16)
    grad_den = -jnp.sum(grad_out * outputs, axis=-1, keepdims=True) / denoms
    grad_both = jnp.concatenate([grad_num, grad_den.astype(BF16)], axis=-1)
    grad_memory = from_others(mul("hcm,hce->hme", phi_q, grad_both), False).astype(BF16)
    grad_scores = jnp.where(
        causal, (mul("hce,hke->hck", grad_num, values) + grad_den).astype(BF16), 0
    )
    grad_q = mul("hck,hkm->hcm", grad_scores, phi_k) + mul("hce,hme->hcm", grad_both, memory)
    grad_k = mul("hck,hcm->hkm", grad_scores, phi_q)
    grad_k = grad_k + mul("hke,hme->hkm", summed_values, grad_memory)
    grad_v = mul("hck,hce->hke", scores, grad_num)
    grad_v = grad_v + mul("hkm,hme->hke", phi_k, grad_memory[..., :-1])
    grad_mixed = jnp.stack(
        [
            join_heads(plain_features_back(queries, projector, expo_q, grad_q)),
            join_heads(plain_features_back(keys, projector, expo_k, grad_k)),
            join_heads(grad_v),
        ]
    ).astype(BF16)
    grad_wqkv = mul("ld,cle->dce", normed, grad_mixed)
    grad_normed = mul("cle,dce->ld", grad_mixed, w_qkv)
    grad_inputs, grad_gain1, grad_shift1 = first_pull(grad_normed)
    grad_tokens = grad_resid + grad_inputs

    tensor, dp = lax.axis_size("tensor"), lax.axis_size("dp")
    wide = grad_wqkv.shape[0]

    def by_owner(grad):
        shaped = grad.reshape(dp, wide // dp, -1, tensor, grad.shape[-1] // tensor)
        moved = jnp.transpose(shaped, (0, 3, 1, 2, 4))
        return moved.reshape(dp * tensor, wide // dp, -1).astype(BF16)

    packed = jnp.concatenate(
        [by_owner(g) for g in (grad_wqkv, grad_wout, grad_up, grad_down)], axis=2
    )
    owned = lax.psum_scatter(packed, ("dp", "tensor"), scatter_dimension=0, tiled=True)[0]
    owned = owned.astype(F32)
    edge = [3 * wide // tensor, 4 * wide // tensor, 4 * wide // tensor + w_up.shape[1] // tensor]
    own_qkv, own_wout, own_up, own_down = jnp.split(owned, edge, axis=1)
    grad_gains, grad_shifts = lax.psum(
        (jnp.stack([grad_gain1, grad_gain2]), jnp.stack([grad_shift1, grad_shift2])),
        ("dp", "tensor"),
    )
    return (
        result,
        grad_tokens,
        own_qkv.reshape(wide // dp, 3, wide // tensor),
        own_wout.T,
        own_up,
        own_down.T,
        grad_gains,
        grad_shifts,
    )


def solution(mesh):
    placed = (
        P(("dp", "tensor"), None),
        P(("dp", "tensor"), None),
        P(None, None, "tensor"),
        P("tensor", None),
        P(None, "tensor"),
        P("tensor", None),
        P(),
        P(),
        P(),
        P(),
        P(),
    )
    return jax.shard_map(
        fused if fits(mesh) else plain,
        mesh=mesh,
        in_specs=placed,
        out_specs=(
            P(("dp", "tensor"), None),
            P(("dp", "tensor"), None),
            P("dp", None, "tensor"),
            P("tensor", "dp"),
            P("dp", "tensor"),
            P("tensor", "dp"),
            P(),
            P(),
        ),
        check_vma=False,
    )
```

```python
import jax
import jax.numpy as jnp
from jax import lax
from jax.experimental import pallas as pl
from jax.experimental.pallas import tpu as pltpu
from jax.sharding import PartitionSpec as P

HEAD_DIM = 64
FEATURES = 256
EPS = 1e-05
F32 = jnp.float32
BF16 = jnp.bfloat16
FACTOR = HEAD_DIM ** (-0.25)
ROWS, WIDE, TILE, FF = 1024, 512, 256, 2048
TILES = ROWS // TILE
PAIRS = 4


def nn(a, b):
    return lax.dot_general(a, b, (((1,), (0,)), ((), ())), preferred_element_type=F32)


def nt(a, b):
    return lax.dot_general(a, b, (((1,), (1,)), ((), ())), preferred_element_type=F32)


def tn(a, b):
    return lax.dot_general(a, b, (((0,), (0,)), ((), ())), preferred_element_type=F32)


def iota(shape, dim):
    return lax.broadcasted_iota(jnp.int32, shape, dim)


def row_tile(t):
    return pl.ds(pl.multiple_of(t * TILE, TILE), TILE)


def lane_tile(j, width=128):
    return pl.ds(pl.multiple_of(j * width, width), width)


def loop(n, body):
    lax.fori_loop(0, n, lambda i, c: (body(i), c)[1], 0)


def of_head(shape, dim, head):
    return (iota(shape, dim) & HEAD_DIM) == head * HEAD_DIM


def centre(v):
    mean = jnp.mean(v, axis=-1, keepdims=True)
    off = v - mean
    rstd = lax.rsqrt(jnp.mean(off * off, axis=-1, keepdims=True) + EPS)
    return off * rstd, rstd


def centre_back(grad, hat, rstd, gain):
    scaled = grad * gain
    first = jnp.mean(scaled, axis=-1, keepdims=True)
    second = jnp.mean(scaled * hat, axis=-1, keepdims=True)
    return rstd * (scaled - first - hat * second)


def gelu_and_slope(u):
    bell = jnp.exp(-0.5 * u * u)
    t = 1.0 / (1.0 + (0.3275911 * 0.7071067811865476) * jnp.abs(u))
    poly = 0.5 * 1.061405429
    for c in (-1.453152027, 1.421413741, -0.284496736, 0.254829592):
        poly = poly * t + 0.5 * c
    tail = poly * t * bell
    cdf = jnp.where(u >= 0, 1.0 - tail, tail)
    return u * cdf, cdf + (0.3989422804014327 * u) * bell


def features_of(rows, wf):
    wide = rows.astype(F32)
    both = jnp.concatenate([rows, ((0.5 * FACTOR) * wide * wide).astype(BF16)], axis=1)
    return (jnp.exp(FACTOR * nn(both, wf)) * FEATURES ** (-0.5)).astype(BF16)


def features_back(rows, wf, weighted):
    through = nt(weighted, wf)
    half = 2 * HEAD_DIM
    return FACTOR * through[:, :half] + (FACTOR * FACTOR) * through[:, half:] * rows.astype(F32)


def merge_heads(state):
    own = of_head((state.shape[0], FEATURES), 0, 0)
    return jnp.where(own, state[:, :FEATURES], state[:, FEATURES:])


class Phases:
    def __init__(self, **refs):
        self.__dict__.update(refs)

    def set_up(self):
        self.vx[:, :, 128:] = jnp.ones((PAIRS, ROWS, 128), BF16)
        fresh, last = self.fresh[...], self.last[...]
        zero = jnp.zeros((HEAD_DIM, FEATURES), BF16)
        minus = jnp.full((HEAD_DIM, FEATURES), -1.0, BF16)
        for j in range(PAIRS):
            for head in range(2):
                flag = (self.flags[2 * j + head] == 1).astype(F32)
                omega = (flag * fresh.astype(F32) + (1.0 - flag) * last.astype(F32)).astype(BF16)
                for lower, block in ((0, omega), (128, minus)):
                    for other in range(2):
                        at = pl.ds(lower + head * HEAD_DIM, HEAD_DIM)
                        col = pl.ds(other * FEATURES, FEATURES)
                        self.wf[j, at, col] = block if other == head else zero
        self.small[...] = jnp.zeros(self.small.shape, F32)

    def norm1(self):
        def body(t):
            hat, _ = centre(self.tokens[row_tile(t), :].astype(F32))
            self.n1[row_tile(t), :] = (hat * self.gains[0:1, :] + self.shifts[0:1, :]).astype(BF16)

        loop(TILES, body)

    def project(self, hh):
        for jj in range(2):
            self.run[jj] = jnp.zeros((TILE, FEATURES), F32)

        def body(t):
            rows = self.n1[row_tile(t), :]
            parts = [
                nn(rows, self.wqkv[hh, c]).astype(BF16) for c in range(3)
            ]
            for jj in range(2):
                j = 2 * hh + jj
                q, k, v = (p[:, jj * 128 : (jj + 1) * 128] for p in parts)
                self.q[j, row_tile(t), :] = q
                self.k[j, row_tile(t), :] = k
                self.vx[j, row_tile(t), 0:128] = v
                wf = self.wf[j]
                self.phi_q[j, row_tile(t), :] = features_of(q, wf)
                phi_k = features_of(k, wf)
                self.phi_k[j, row_tile(t), :] = phi_k
                state = merge_heads(tn(self.vx[j, row_tile(t), :], phi_k))
                self.zt[j * TILES + t] = state.astype(BF16)
                self.run[jj] += state

        loop(TILES, body)
        for jj in range(2):
            self.pack(self.zsend, 2 * hh + jj, self.run.at[jj], False)

    def pack(self, out, j, state, gradient):
        first, second = state[128:136, :], state[192:200, :]
        if gradient:
            first = 0.5 * (first + state[160:168, :])
            second = 0.5 * (second + state[224:232, :])
        out[j, 0:128, :] = state[0:128, :].astype(BF16)
        out[j, 128:136, :] = first.astype(BF16)
        out[j, 136:144, :] = second.astype(BF16)

    def unpack(self, packed):
        low = packed.astype(F32)
        sums = [jnp.broadcast_to(low[r : r + 1], (HEAD_DIM, FEATURES)) for r in (128, 136)]
        return jnp.concatenate([low[0:128], *sums], axis=0)

    def attend_near(self, hh):
        for jj in range(2):
            j = 2 * hh + jj

            def body(t, j=j):
                at = row_tile(t)
                vx = self.vx[j, at, :]
                both = []
                for head in range(2):
                    f = slice(head * FEATURES, (head + 1) * FEATURES)
                    s = nt(self.phi_q[j, at, f], self.phi_k[j, at, f])
                    s = jnp.where(iota(s.shape, 1) <= iota(s.shape, 0), s, 0.0).astype(BF16)
                    both.append(nn(s, vx))
                r = jnp.where(of_head(both[0].shape, 1, 0), both[0], both[1])
                self.out[at, lane_tile(j)] = r[:, :128]
                self.grad[at, lane_tile(j)] = r[:, 128:]

            loop(TILES, body)

    def attend_far(self, j, start):
        self.run[0] = start(j)

        def body(t):
            at = row_tile(t)
            before = self.run[0]
            low = before.astype(BF16)
            self.run[0] = before + self.zt[j * TILES + t].astype(F32)
            self.zt[j * TILES + t] = low
            both = [
                nt(self.phi_q[j, at, head * FEATURES : (head + 1) * FEATURES], low)
                for head in range(2)
            ]
            r = jnp.where(of_head(both[0].shape, 1, 0), both[0], both[1])
            inverse = 1.0 / (r[:, 128:] + self.grad[at, lane_tile(j)])
            num = r[:, :128] + self.out[at, lane_tile(j)]
            self.a[at, lane_tile(j)] = (num * inverse).astype(BF16)
            self.inverse[j, at, :] = inverse

        loop(TILES, body)

    def norm2(self):
        def body(t):
            at = row_tile(t)
            w_out = self.wout[...].reshape(WIDE, WIDE)
            h = self.tokens[at, :].astype(F32) + nn(self.a[at, :], w_out)
            self.out[at, :] = h
            hat, rstd = centre(h)
            self.hat2[at, :] = hat.astype(BF16)
            self.rstd2[at, :] = jnp.broadcast_to(rstd, (TILE, 128))
            self.n2[at, :] = (hat * self.gains[1:2, :] + self.shifts[1:2, :]).astype(BF16)
            self.grad[at, :] = jnp.zeros((TILE, WIDE), F32)

        loop(TILES, body)

    def feed(self, slot, first, count):
        def body(n):
            i = first + n
            t, p = lax.div(i, 2), lax.rem(i, 2)
            at, cols = row_tile(t), lane_tile(p, 512)
            w_up, w_down = self.wup[slot, :, cols], self.wdown[slot, cols, :]
            g, slope = gelu_and_slope(nn(self.n2[at, :], w_up))
            g = g.astype(BF16)
            du = (slope * nt(self.cot[at, :], w_down)).astype(BF16)
            self.g[t * 4 + slot * 2 + p] = g
            self.du[t * 4 + slot * 2 + p] = du
            self.out[at, :] += nn(g, w_down)
            self.grad[at, :] += nt(du, w_up)

        loop(count, body)

    def norm2_back(self):
        def body(t):
            at = row_tile(t)
            grad, hat = self.grad[at, :], self.hat2[at, :].astype(F32)
            self.small[1:2, :] += jnp.sum(grad * hat, axis=0, keepdims=True)
            self.small[3:4, :] += jnp.sum(grad, axis=0, keepdims=True)
            back = centre_back(grad, hat, self.rstd2[at, 0:1], self.gains[1:2, :])
            dh = self.cot[at, :].astype(F32) + back
            self.grad[at, :] = dh
            self.dhb[at, :] = dh.astype(BF16)

        loop(TILES, body)

    def flip(self, source, out):
        def body(t):
            out[:, row_tile(t)] = source[row_tile(t), :].T

        loop(TILES, body)

    def weight_grad(self, xt, blocks, n_cols, store):
        def body(c):
            total = nn(xt[:, 0:TILE], blocks(0, c))
            for t in range(1, TILES):
                total = total + nn(xt[:, t * TILE : (t + 1) * TILE], blocks(t, c))
            store(c, total)

        loop(n_cols, body)

    def attend_back_start(self):
        def body(t):
            at = row_tile(t)
            w_out = self.wout[...].reshape(WIDE, WIDE)
            da = nt(self.dhb[at, :], w_out)
            o = self.a[at, :].astype(F32)
            same = (iota((128, 128), 0) & HEAD_DIM) == (iota((128, 128), 1) & HEAD_DIM)
            ones = jnp.where(same, 1.0, 0.0).astype(BF16)
            high = (iota((TILE, 128), 1) & 32) == 0
            for j in range(PAIRS):
                lanes = slice(j * 128, (j + 1) * 128)
                do, inverse = da[:, lanes], self.inverse[j, at, :]
                dden = -nn((do * o[:, lanes]).astype(BF16), ones) * inverse
                top = dden.astype(BF16)
                rest = (dden - top.astype(F32)).astype(BF16)
                self.dnx[j, at, 0:128] = (do * inverse).astype(BF16)
                self.dnx[j, at, 128:] = jnp.where(high, top, rest) * jnp.asarray(1 / 32, BF16)

        loop(TILES, body)

    def sums_back(self, j):
        self.run[0] = jnp.zeros((TILE, FEATURES), F32)

        def body(t):
            at = row_tile(t)
            state = merge_heads(tn(self.dnx[j, at, :], self.phi_q[j, at, :]))
            self.gt[j * TILES + t] = state.astype(BF16)
            self.run[0] += state

        loop(TILES, body)
        self.pack(self.gsend, j, self.run.at[0], True)

    def back_q(self, j):
        def body(t):
            at = row_tile(t)
            dnx = self.dnx[j, at, :]
            w = []
            for head in range(2):
                f = slice(head * FEATURES, (head + 1) * FEATURES)
                own = jnp.where(of_head(dnx.shape, 1, head), dnx, jnp.zeros_like(dnx))
                ds = nt(own, self.vx[j, at, :])
                ds = jnp.where(iota(ds.shape, 1) <= iota(ds.shape, 0), ds, 0.0).astype(BF16)
                dphi = nn(ds, self.phi_k[j, at, f]) + nn(own, self.zt[j * TILES + t])
                w.append((dphi * self.phi_q[j, at, f].astype(F32)).astype(BF16))
            dq = features_back(self.q[j, at, :], self.wf[j], jnp.concatenate(w, axis=1))
            self.dqkv[0 * TILES + t, :, lane_tile(j)] = dq.astype(BF16)

        loop(TILES, body)

    def back_kv(self, j, start):
        self.run[0] = start(j)

        def body(i):
            t = TILES - 1 - i
            at = row_tile(t)
            after = self.run[0]
            low = after.astype(BF16)
            self.run[0] = after + self.gt[j * TILES + t].astype(F32)
            dnx, vx = self.dnx[j, at, :], self.vx[j, at, :]
            w, dv = [], []
            for head in range(2):
                f = slice(head * FEATURES, (head + 1) * FEATURES)
                phi_q, phi_k = self.phi_q[j, at, f], self.phi_k[j, at, f]
                st = nt(phi_k, phi_q)
                upper = iota(st.shape, 0) <= iota(st.shape, 1)
                st = jnp.where(upper, st, 0.0).astype(BF16)
                own = jnp.where(of_head(vx.shape, 1, head), vx, jnp.zeros_like(vx))
                dst = nt(own, dnx)
                dst = jnp.where(upper, dst, 0.0).astype(BF16)
                dphi = nn(dst, phi_q) + nn(own, low)
                w.append((dphi * phi_k.astype(F32)).astype(BF16))
                dv.append(nn(st, dnx[:, 0:128]) + nt(phi_k, low[0:128]))
            dk = features_back(self.k[j, at, :], self.wf[j], jnp.concatenate(w, axis=1))
            self.dqkv[1 * TILES + t, :, lane_tile(j)] = dk.astype(BF16)
            dv = jnp.where(of_head(dv[0].shape, 1, 0), dv[0], dv[1])
            self.dqkv[2 * TILES + t, :, lane_tile(j)] = dv.astype(BF16)

        loop(TILES, body)

    def norm1_back(self, first, count):
        def body(n):
            t = first + n
            at = row_tile(t)
            grad = jnp.zeros((TILE, WIDE), F32)
            for hh in range(2):
                for c in range(3):
                    part = self.dqkv[c * TILES + t, :, hh * 256 : (hh + 1) * 256]
                    grad = grad + nt(part, self.wqkv[hh, c])
            hat, rstd = centre(self.tokens[at, :].astype(F32))
            self.small[0:1, :] += jnp.sum(grad * hat, axis=0, keepdims=True)
            self.small[2:3, :] += jnp.sum(grad, axis=0, keepdims=True)
            self.grad[at, :] += centre_back(grad, hat, rstd, self.gains[0:1, :])

        loop(count, body)


def work_buffers():
    vmem = pltpu.VMEM
    return dict(
        n1=vmem((ROWS, WIDE), BF16),
        q=vmem((PAIRS, ROWS, 128), BF16),
        k=vmem((PAIRS, ROWS, 128), BF16),
        vx=vmem((PAIRS, ROWS, 256), BF16),
        phi_q=vmem((PAIRS, ROWS, 512), BF16),
        phi_k=vmem((PAIRS, ROWS, 512), BF16),
        zt=vmem((PAIRS * TILES, 256, 256), BF16),
        gt=vmem((PAIRS * TILES, 256, 256), BF16),
        run=vmem((2, 256, 256), F32),
        wf=vmem((PAIRS, 256, 512), BF16),
        a=vmem((ROWS, WIDE), BF16),
        inverse=vmem((PAIRS, ROWS, 128), F32),
        n2=vmem((ROWS, WIDE), BF16),
        hat2=vmem((ROWS, WIDE), BF16),
        rstd2=vmem((ROWS, 128), F32),
        g=vmem((TILES * 4, 256, 512), BF16),
        du=vmem((TILES * 4, 256, 512), BF16),
        dnx=vmem((PAIRS, ROWS, 256), BF16),
        zsend=vmem((PAIRS, 144, 256), BF16),
        gsend=vmem((PAIRS, 144, 256), BF16),
        xt=vmem((WIDE, ROWS), BF16),
        xt2=vmem((WIDE, ROWS), BF16),
    )


MESH = pl.DeviceIdType.MESH
OWNED = 1024


class Links:
    def __init__(self, deep, refs):
        self.deep = deep
        self.__dict__.update(refs)
        self.dp, self.me = lax.axis_index("dp"), lax.axis_index("tensor")
        self.core = lax.rem(self.dp, 2)
        self.x = lax.rem(lax.div(self.dp, 2), 2)
        self.z = lax.div(self.dp, 4)
        self.block = WIDE // (4 * deep)

    def place(self, axis, step=1):
        dp, me = self.dp, self.me
        if axis == "core":
            return dict(dp=dp + 1 - 2 * self.core, tensor=me)
        if axis == "x":
            return dict(dp=dp + 2 - 4 * self.x, tensor=me)
        if axis == "y":
            return dict(dp=dp, tensor=1 - me)
        return dict(dp=dp + 4 * (lax.rem(self.z + step, self.deep) - self.z), tensor=me)

    def partners(self):
        steps = [self.place("z", s) for s in range(1, self.deep)]
        return [self.place(a) for a in ("core", "x", "y")] + steps

    def greet(self):
        barrier = pltpu.get_barrier_semaphore()
        for where in self.partners():
            pl.semaphore_signal(barrier, inc=1, device_id=where, device_id_type=MESH)

    def met(self):
        pl.semaphore_wait(pltpu.get_barrier_semaphore(), len(self.partners()))

    def copy(self, source, target, sems, at, where):
        return pltpu.make_async_remote_copy(
            src_ref=source,
            dst_ref=target,
            send_sem=sems.at[2 * at],
            recv_sem=sems.at[2 * at + 1],
            device_id=where,
            device_id_type=MESH,
        )


    def parts(self, i):
        source = (self.wqkv_in, self.wout_in, self.wup_in, self.wdown_in)[i]
        slots = (self.wqkv, self.wout, self.wup, self.wdown)[i]
        size = source.shape[-2] // (2 if i < 2 else 4)

        def cut(ref, p):
            here = pl.ds(pl.multiple_of(p * size, size), size)
            return ref.at[:, here] if i == 0 else ref.at[here]

        return source, slots, cut

    def part(self, i, far=False):
        if i < 2:
            return self.core
        return 2 * ((1 - self.x) if far else self.x) + self.core

    def own_weight(self, i):
        source, slots, _ = self.parts(i)
        return pltpu.make_async_copy(source, slots.at[self.me], self.own_sems.at[i])

    def over(self, i):
        source, slots, cut = self.parts(i)
        p = self.part(i)
        target = cut(slots.at[self.me], p)
        return self.copy(cut(source, p), target, self.over_sems, i, self.place("y"))

    def across(self, i):
        _, slots, cut = self.parts(i)
        held = cut(slots.at[1 - self.me], self.part(i))
        return self.copy(held, held, self.across_sems, i - 2, self.place("x"))

    def along(self, i, far=False):
        _, slots, cut = self.parts(i)
        held = cut(slots.at[1 - self.me], self.part(i, far))
        return self.copy(held, held, self.along_sems, i + (2 if far else 0), self.place("core"))


    def axes(self, seg):
        return ("y", "x") if seg % 2 == 0 else ("x", "y")

    def index(self, axis):
        return self.me if axis == "y" else self.x

    def stage(self, seg, depth):
        grads = self.grads[seg]
        if depth == 0:
            source = grads.at[1 - self.core]
            return self.copy(source, self.got[seg][0], self.sum_sems[seg], 0, self.place("core"))
        axis = self.axes(seg)[depth - 1]
        start, size = self.span(seg, depth, 1 - self.index(axis))
        source = grads.at[self.core, pl.ds(pl.multiple_of(start, self.block), size)]
        return self.copy(source, self.got[seg][depth], self.sum_sems[seg], depth, self.place(axis))

    def span(self, seg, depth, last):
        start, size = 0, WIDE
        for i in range(depth):
            size = size // 2
            at = last if i == depth - 1 else self.index(self.axes(seg)[i])
            start = start + at * size
        return start, size

    def mine(self, seg, depth):
        if depth == 0:
            return 0, WIDE
        return self.span(seg, depth, self.index(self.axes(seg)[depth - 1]))

    def start(self, seg, depth):
        self.stage(seg, depth).start()

    def finish(self, seg, depth):
        self.stage(seg, depth).wait()
        start, size = self.mine(seg, depth)
        grads, got = self.grads[seg], self.got[seg][depth]
        step = min(size, 64)

        def body(i):
            there = pl.ds(pl.multiple_of(i * step, step), step)
            here = pl.ds(pl.multiple_of(start + i * step, step), step)
            grads[self.core, here] = grads[self.core, here] + got[there]

        loop(size // step, body)

    def z_copy(self, seg, step):
        start, _ = self.mine(seg, 2)
        row = start + lax.rem(self.z + step, self.deep) * self.block
        source = self.grads[seg].at[self.core, pl.ds(pl.multiple_of(row, self.block), self.block)]
        target = self.got[seg][3].at[step - 1]
        return self.copy(source, target, self.sum_sems[seg], 2 + step, self.place("z", step))

    def start_z(self, seg):
        for step in range(1, self.deep):
            self.z_copy(seg, step).start()

    def finish_z(self, seg):
        start, _ = self.mine(seg, 2)
        here = pl.ds(pl.multiple_of(start + self.z * self.block, self.block), self.block)
        total = self.grads[seg][self.core, here].astype(F32)
        for step in range(1, self.deep):
            self.z_copy(seg, step).wait()
            total = total + self.got[seg][3][step - 1].astype(F32)
        return total


    def small_copies(self, stage):
        if stage < 3:
            places = [self.place(("core", "y", "x")[stage])]
        else:
            places = [self.place("z", s) for s in range(1, self.deep)]
        return [
            self.copy(self.small.at[stage], self.heard.at[stage + n], self.small_sems, stage + n, where)
            for n, where in enumerate(places)
        ]

    def small_start(self, stage):
        for both in self.small_copies(stage):
            both.start()

    def small_finish(self, stage):
        total = self.small[stage]
        for n, both in enumerate(self.small_copies(stage)):
            both.wait()
            total = total + self.heard[stage + n]
        self.small[stage + 1] = total


def by_owner(ref, flipped, deep, total, tensor, lanes):
    block = WIDE // (4 * deep)
    low = total.astype(BF16)
    for d in range(4 * deep):
        core, x, z = d % 2, d // 2 % 2, d // 4
        near, far = (x, tensor) if flipped else (tensor, x)
        row = ((near * 2 + far) * deep + z) * block
        here = pl.ds(pl.multiple_of(row, block), block)
        ref[core, here, lanes] = low[d * block : (d + 1) * block]


def layer_kernel(deep, names, *refs):
    r = dict(zip(names, refs))
    sends = r["sum_sems"]
    links = Links(
        deep,
        dict(
            r,
            grads=tuple(r[f"grads{s}"] for s in range(4)),
            got=tuple(tuple(r[f"got{s}_{d}"] for d in range(4)) for s in range(4)),
            sum_sems=tuple(sends.at[s] for s in range(4)),
        ),
    )
    p = Phases(**dict(r, dqkv=r["du"], dhb=r["hat2"], small=r["small"].at[0]))
    me = links.me
    other = 1 - me

    links.greet()
    for i in range(4):
        links.own_weight(i).start()
    cot_in = pltpu.make_async_copy(r["cot_in"], p.cot, r["io_sems"].at[0])
    cot_in.start()
    p.set_up()
    links.met()
    for i in range(2):
        links.over(i).start()
    p.norm1()
    links.own_weight(0).wait()
    p.project(me)

    def z_copy(hh):
        here = pl.ds(2 * hh, 2)
        return links.copy(p.zsend.at[here], p.zgot.at[here], r["z_sems"], hh, links.place("y"))

    @pl.when(me == 0)
    def _():
        p.zgot[...] = jnp.zeros(p.zgot.shape, BF16)
        z_copy(0).start()

    @pl.when(me == 1)
    def _():
        p.ggot[...] = jnp.zeros(p.ggot.shape, BF16)

    links.over(2).start()
    p.attend_near(me)
    links.over(0).wait()
    links.along(0).start()
    links.along(0).wait()
    p.project(other)

    @pl.when(me == 0)
    def _():
        z_copy(1).start()

    links.over(3).start()
    links.over(1).wait()
    links.along(1).start()
    p.attend_near(other)
    links.over(2).wait()
    links.across(2).start()
    links.along(2).start()
    for hh in range(2):

        @pl.when(me == 1)
        def _():
            z_copy(hh).wait_recv()

        for jj in range(2):
            p.attend_far(2 * hh + jj, lambda j: p.unpack(p.zgot[j]))

        @pl.when(me == 0)
        def _():
            z_copy(hh).wait_send()

    links.own_weight(1).wait()
    links.along(1).wait()
    p.norm2()
    links.own_weight(2).wait()
    links.own_weight(3).wait()
    cot_in.wait()
    p.feed(me, 0, 4)
    links.across(2).wait()
    links.along(2, True).start()
    links.over(3).wait()
    links.across(3).start()
    links.along(3).start()
    p.feed(me, 4, 4)
    links.across(3).wait()
    links.along(3, True).start()
    for i in range(2, 4):
        links.along(i).wait()
        links.along(i, True).wait()
    p.feed(other, 0, 8)
    out_copy = pltpu.make_async_copy(p.out, r["out_hbm"], r["io_sems"].at[1])
    out_copy.start()

    p.norm2_back()
    p.attend_back_start()
    loop(PAIRS, p.sums_back)
    g_copy = links.copy(p.gsend, p.ggot, r["g_sems"], 0, links.place("y"))

    @pl.when(me == 1)
    def _():
        g_copy.start()

    def ff_grad(xt, blocks, seg):
        def store(c, total):
            lanes = lane_tile(lax.rem(c, 4), TILE)
            by_owner(links.grads[seg], seg == 1, deep, total, lax.div(c, 4), lanes)

        def take(t, c):
            return blocks[t * 4 + lax.div(c, 2), :, lane_tile(lax.rem(c, 2), TILE)]

        p.weight_grad(xt, take, 8, store)

    p.flip(p.n2, p.xt)
    ff_grad(p.xt, p.du, 0)
    links.start(0, 0)
    p.flip(p.cot, p.xt2)
    ff_grad(p.xt2, p.g, 1)
    links.start(1, 0)
    links.finish(0, 0)
    links.start(0, 1)
    p.flip(p.dhb, p.xt)
    p.weight_grad(
        p.xt,
        lambda t, c: p.a[pl.ds(t * TILE, TILE), lane_tile(c, TILE)],
        2,
        lambda c, total: by_owner(links.grads[2], False, deep, total, c, slice(0, TILE)),
    )
    links.finish(1, 0)
    links.start(1, 1)
    p.flip(p.n1, p.xt2)
    loop(PAIRS, p.back_q)
    for seg in range(2):
        links.finish(seg, 1)
        links.start(seg, 2)

    @pl.when(me == 0)
    def _():
        g_copy.wait_recv()

    @pl.when(me == 1)
    def _():
        g_copy.wait_send()

    def back(j):
        p.back_kv(j, lambda j: p.unpack(p.ggot[j]))

    def qkv_grad(seg):
        pieces = [(hh, c) for hh in range(2) for c in range(3)]
        base = (0, 0, TILE, 0)[seg]
        for n in range(3):
            total = jnp.zeros((WIDE, TILE), F32)
            for t in range(TILES):
                rows = [
                    p.dqkv[c * TILES + t, :, lane_tile(2 * hh + seg - 2)]
                    for hh, c in pieces[2 * n : 2 * n + 2]
                ]
                total = total + nn(
                    p.xt2[:, t * TILE : (t + 1) * TILE], jnp.concatenate(rows, axis=1)
                )
            for half, (hh, c) in enumerate(pieces[2 * n : 2 * n + 2]):
                by_owner(
                    links.grads[seg],
                    seg == 3,
                    deep,
                    total[:, half * 128 : (half + 1) * 128],
                    hh,
                    pl.ds(base + c * 128, 128),
                )

    back(0)
    back(2)
    for seg in range(2):
        links.finish(seg, 2)
        links.start_z(seg)
    qkv_grad(2)
    links.start(2, 0)
    back(1)
    links.finish(2, 0)
    links.start(2, 1)
    back(3)
    qkv_grad(3)
    links.start(3, 0)
    r["own_up"][...] = links.finish_z(0)
    r["own_down"][...] = links.finish_z(1)
    p.norm1_back(0, 2)
    links.finish(3, 0)
    links.start(3, 1)
    p.norm1_back(2, 2)
    grad_copy = pltpu.make_async_copy(p.grad, r["grad_hbm"], r["io_sems"].at[2])
    grad_copy.start()
    links.small_start(0)
    links.finish(2, 1)
    links.start(2, 2)
    links.small_finish(0)
    links.small_start(1)
    links.finish(3, 1)
    links.start(3, 2)
    links.small_finish(1)
    links.small_start(2)
    links.finish(2, 2)
    links.start_z(2)
    links.finish(3, 2)
    links.start_z(3)
    links.small_finish(2)
    links.small_start(3)

    def own_qkv(total, jj):
        for c in range(3):
            r["own_qkv"][c, :, jj * 128 : (jj + 1) * 128] = total[:, c * 128 : (c + 1) * 128]

    total = links.finish_z(2)
    r["own_wout"][...] = total[:, :TILE]
    own_qkv(total[:, TILE:], 0)
    own_qkv(links.finish_z(3), 1)
    links.small_finish(3)
    r["own_gains"][...] = r["small"][4, 0:2]
    r["own_shifts"][...] = r["small"][4, 2:4]
    out_copy.wait()
    grad_copy.wait()


def layer_call(deep, tokens, cotangent, wqkv, wout, wup, wdown, gains, shifts, fresh, last, flags):
    vmem, hbm = pltpu.VMEM, pl.ANY
    block = WIDE // (4 * deep)
    inputs = dict(
        tokens=(tokens, vmem),
        cot_in=(cotangent, hbm),
        wqkv_in=(wqkv, hbm),
        wout_in=(wout, hbm),
        wup_in=(wup, hbm),
        wdown_in=(wdown, hbm),
        gains=(gains, vmem),
        shifts=(shifts, vmem),
        fresh=(fresh, vmem),
        last=(last, vmem),
        flags=(flags, pltpu.SMEM),
    )
    outputs = dict(
        out_hbm=((ROWS, WIDE), hbm),
        grad_hbm=((ROWS, WIDE), hbm),
        own_qkv=((3, block, 256), vmem),
        own_wout=((block, 256), vmem),
        own_up=((block, 1024), vmem),
        own_down=((block, 1024), vmem),
        own_gains=((2, WIDE), vmem),
        own_shifts=((2, WIDE), vmem),
    )
    dma = pltpu.SemaphoreType.DMA
    widths = (1024, 1024, 640, 384)
    scratch = dict(
        work_buffers(),
        out=vmem((ROWS, WIDE), F32),
        grad=vmem((ROWS, WIDE), F32),
        cot=vmem((ROWS, WIDE), BF16),
        wqkv=vmem((2, 3, WIDE, 256), BF16),
        wout=vmem((2, 256, WIDE), BF16),
        wup=vmem((2, WIDE, 1024), BF16),
        wdown=vmem((2, 1024, WIDE), BF16),
        zgot=vmem((PAIRS, 144, 256), BF16),
        ggot=vmem((PAIRS, 144, 256), BF16),
        small=vmem((5, 4, WIDE), F32),
        heard=vmem((2 + deep, 4, WIDE), F32),
        own_sems=dma((4,)),
        over_sems=dma((8,)),
        across_sems=dma((4,)),
        along_sems=dma((12,)),
        z_sems=dma((4,)),
        g_sems=dma((2,)),
        io_sems=dma((3,)),
        sum_sems=dma((4, 2 * (2 + deep))),
        small_sems=dma((2 * (2 + deep),)),
    )
    for seg, width in enumerate(widths):
        scratch[f"grads{seg}"] = vmem((2, WIDE, width), BF16)
        for depth in range(3):
            scratch[f"got{seg}_{depth}"] = vmem((WIDE // 2**depth, width), BF16)
        scratch[f"got{seg}_3"] = vmem((deep - 1, block, width), BF16)
    names = (*inputs, *outputs, *scratch)

    def kernel(*refs):
        layer_kernel(deep, names, *refs)

    return pl.pallas_call(
        kernel,
        out_shape=tuple(jax.ShapeDtypeStruct(shape, F32) for shape, _ in outputs.values()),
        in_specs=[pl.BlockSpec(memory_space=space) for _, space in inputs.values()],
        out_specs=tuple(pl.BlockSpec(memory_space=space) for _, space in outputs.values()),
        scratch_shapes=list(scratch.values()),
        compiler_params=pltpu.CompilerParams(
            collective_id=0, has_side_effects=True, vmem_limit_bytes=67043328
        ),
        name="layer",
    )(*(array for array, _ in inputs.values()))


def fused(
    tokens, cotangent, w_qkv, w_out, w_up, w_down, gains, shifts, feat_fresh, feat_last, flags
):
    deep = lax.axis_size("dp") // 4
    by_part = jnp.transpose(w_qkv, (1, 0, 2))
    outs = layer_call(
        deep,
        tokens,
        cotangent,
        by_part,
        w_out,
        w_up,
        w_down,
        gains,
        shifts,
        feat_fresh,
        feat_last,
        flags,
    )
    result, grad_tokens, own_qkv, own_wout, own_up, own_down, own_gains, own_shifts = outs
    return (
        result,
        grad_tokens,
        jnp.transpose(own_qkv, (1, 0, 2)),
        own_wout.T,
        own_up,
        own_down.T,
        own_gains,
        own_shifts,
    )


def fits(mesh):
    return mesh.shape["tensor"] == 2 and mesh.shape["dp"] % 4 == 0 and mesh.shape["dp"] <= 64


def normalize(inputs, norm_gain, offset):
    average = jnp.mean(inputs, axis=-1, keepdims=True)
    centered = inputs - average
    variance = jnp.mean(centered * centered, axis=-1, keepdims=True)
    return centered * lax.rsqrt(variance + EPS) * norm_gain + offset


def gelu_exact(inputs):
    return jax.nn.gelu(inputs, approximate=False)


def mul(spec, *operands):
    return jnp.einsum(spec, *operands, preferred_element_type=F32)


def split_heads(matrix):
    length = matrix.shape[0]
    return jnp.transpose(matrix.reshape(length, -1, HEAD_DIM), (1, 0, 2))


def join_heads(stacked):
    moved = jnp.transpose(stacked, (1, 0, 2))
    return moved.reshape(moved.shape[0], -1)


def plain_features(inputs, projector):
    factor = HEAD_DIM ** (-0.25)
    projected = mul("hlc,hcm->hlm", inputs, projector)
    wide_in = inputs.astype(F32)
    squares = 0.5 * factor * factor * jnp.sum(wide_in * wide_in, axis=-1, keepdims=True)
    return jnp.exp(factor * projected - squares) * FEATURES ** (-0.5)


def plain_features_back(inputs, projector, expo, grad_phi):
    factor = HEAD_DIM ** (-0.25)
    grad_pre = grad_phi * expo
    grad_proj = (factor * grad_pre).astype(BF16)
    through = mul("hlm,hcm->hlc", grad_proj, projector)
    return through - factor * factor * jnp.sum(grad_pre, axis=-1, keepdims=True) * inputs.astype(F32)


def from_others(part, before):
    parts = lax.all_gather(part, "tensor")
    mine = lax.axis_index("tensor")
    place = jnp.arange(parts.shape[0])
    taken = (place < mine) if before else (place > mine)
    return jnp.sum(jnp.where(taken[:, None, None, None], parts, 0.0), axis=0)


def with_sums(values):
    return jnp.concatenate([values, jnp.ones_like(values[..., :1])], axis=-1)


def plain(
    tokens, cotangent, w_qkv, w_out, w_up, w_down, gains, shifts, feat_fresh, feat_last, flags
):
    w_qkv = lax.all_gather(w_qkv, "tensor", axis=2, tiled=True)
    w_out = lax.all_gather(w_out, "tensor", axis=0, tiled=True)
    w_up = lax.all_gather(w_up, "tensor", axis=1, tiled=True)
    w_down = lax.all_gather(w_down, "tensor", axis=0, tiled=True)
    inputs = tokens.astype(F32)
    rows = inputs.shape[0]
    normed, first_pull = jax.vjp(normalize, inputs, gains[0], shifts[0])
    normed = normed.astype(BF16)
    projector = jnp.where((flags == 1)[:, None, None], feat_fresh[None], feat_last[None])
    mixed = mul("ld,dce->cle", normed, w_qkv).astype(BF16)
    queries, keys, values = (split_heads(mixed[c]) for c in range(3))
    expo_q, expo_k = plain_features(queries, projector), plain_features(keys, projector)
    phi_q, phi_k = expo_q.astype(BF16), expo_k.astype(BF16)
    summed_values = with_sums(values)
    memory = from_others(mul("hkm,hke->hme", phi_k, summed_values), True).astype(BF16)
    causal = jnp.tril(jnp.ones((rows, rows), jnp.bool_))
    scores = jnp.where(causal, mul("hcm,hkm->hck", phi_q, phi_k), 0.0).astype(BF16)
    both = mul("hck,hke->hce", scores, summed_values) + mul("hcm,hme->hce", phi_q, memory)
    denoms = both[..., -1:]
    outputs = both[..., :-1] / denoms
    joined = join_heads(outputs).astype(BF16)
    residual = inputs + mul("le,ed->ld", joined, w_out)
    second, second_pull = jax.vjp(normalize, residual, gains[1], shifts[1])
    second = second.astype(BF16)
    pre_act = mul("ld,df->lf", second, w_up)
    activated, gelu_pull = jax.vjp(gelu_exact, pre_act)
    act_low = activated.astype(BF16)
    result = residual + mul("lf,fd->ld", act_low, w_down)
    grad_act = mul("ld,fd->lf", cotangent, w_down)
    grad_pre = gelu_pull(grad_act)[0].astype(BF16)
    grad_down = mul("ld,lf->df", cotangent, act_low)
    grad_up = mul("ld,lf->df", second, grad_pre)
    grad_resid, grad_gain2, grad_shift2 = second_pull(mul("lf,df->ld", grad_pre, w_up))
    grad_resid = grad_resid + cotangent.astype(F32)
    resid_low = grad_resid.astype(BF16)
    grad_out = split_heads(mul("ld,ed->le", resid_low, w_out))
    grad_wout = mul("ld,le->de", resid_low, joined)
    grad_num = (grad_out / denoms).astype(BF16)
    grad_den = -jnp.sum(grad_out * outputs, axis=-1, keepdims=True) / denoms
    grad_both = jnp.concatenate([grad_num, grad_den.astype(BF16)], axis=-1)
    grad_memory = from_others(mul("hcm,hce->hme", phi_q, grad_both), False).astype(BF16)
    grad_scores = jnp.where(
        causal, (mul("hce,hke->hck", grad_num, values) + grad_den).astype(BF16), 0
    )
    grad_q = mul("hck,hkm->hcm", grad_scores, phi_k) + mul("hce,hme->hcm", grad_both, memory)
    grad_k = mul("hck,hcm->hkm", grad_scores, phi_q)
    grad_k = grad_k + mul("hke,hme->hkm", summed_values, grad_memory)
    grad_v = mul("hck,hce->hke", scores, grad_num)
    grad_v = grad_v + mul("hkm,hme->hke", phi_k, grad_memory[..., :-1])
    grad_mixed = jnp.stack(
        [
            join_heads(plain_features_back(queries, projector, expo_q, grad_q)),
            join_heads(plain_features_back(keys, projector, expo_k, grad_k)),
            join_heads(grad_v),
        ]
    ).astype(BF16)
    grad_wqkv = mul("ld,cle->dce", normed, grad_mixed)
    grad_normed = mul("cle,dce->ld", grad_mixed, w_qkv)
    grad_inputs, grad_gain1, grad_shift1 = first_pull(grad_normed)
    grad_tokens = grad_resid + grad_inputs

    tensor, dp = lax.axis_size("tensor"), lax.axis_size("dp")
    wide = grad_wqkv.shape[0]

    def by_owner(grad):
        shaped = grad.reshape(dp, wide // dp, -1, tensor, grad.shape[-1] // tensor)
        moved = jnp.transpose(shaped, (0, 3, 1, 2, 4))
        return moved.reshape(dp * tensor, wide // dp, -1).astype(BF16)

    packed = jnp.concatenate(
        [by_owner(g) for g in (grad_wqkv, grad_wout, grad_up, grad_down)], axis=2
    )
    owned = lax.psum_scatter(packed, ("dp", "tensor"), scatter_dimension=0, tiled=True)[0]
    owned = owned.astype(F32)
    edge = [3 * wide // tensor, 4 * wide // tensor, 4 * wide // tensor + w_up.shape[1] // tensor]
    own_qkv, own_wout, own_up, own_down = jnp.split(owned, edge, axis=1)
    grad_gains, grad_shifts = lax.psum(
        (jnp.stack([grad_gain1, grad_gain2]), jnp.stack([grad_shift1, grad_shift2])),
        ("dp", "tensor"),
    )
    return (
        result,
        grad_tokens,
        own_qkv.reshape(wide // dp, 3, wide // tensor),
        own_wout.T,
        own_up,
        own_down.T,
        grad_gains,
        grad_shifts,
    )


def solution(mesh):
    placed = (
        P(("dp", "tensor"), None),
        P(("dp", "tensor"), None),
        P(None, None, "tensor"),
        P("tensor", None),
        P(None, "tensor"),
        P("tensor", None),
        P(),
        P(),
        P(),
        P(),
        P(),
    )
    return jax.shard_map(
        fused if fits(mesh) else plain,
        mesh=mesh,
        in_specs=placed,
        out_specs=(
            P(("dp", "tensor"), None),
            P(("dp", "tensor"), None),
            P("dp", None, "tensor"),
            P("tensor", "dp"),
            P("dp", "tensor"),
            P("tensor", "dp"),
            P(),
            P(),
        ),
        check_vma=False,
    )
```

```python
import jax
import jax.numpy as jnp
from jax import lax
from jax.experimental import pallas as pl
from jax.experimental.pallas import tpu as pltpu
from jax.sharding import PartitionSpec as P

HEAD_DIM = 64
FEATURES = 256
EPS = 1e-05
F32 = jnp.float32
BF16 = jnp.bfloat16
FACTOR = HEAD_DIM ** (-0.25)
ROWS, WIDE, TILE, FF = 1024, 512, 256, 2048
TILES = ROWS // TILE
PAIRS = 4


def nn(a, b):
    return lax.dot_general(a, b, (((1,), (0,)), ((), ())), preferred_element_type=F32)


def nt(a, b):
    return lax.dot_general(a, b, (((1,), (1,)), ((), ())), preferred_element_type=F32)


def tn(a, b):
    return lax.dot_general(a, b, (((0,), (0,)), ((), ())), preferred_element_type=F32)


def iota(shape, dim):
    return lax.broadcasted_iota(jnp.int32, shape, dim)


def row_tile(t, size=TILE):
    return pl.ds(pl.multiple_of(t * size, size), size)


def lane_tile(j, width=128):
    return pl.ds(pl.multiple_of(j * width, width), width)


def loop(n, body):
    lax.fori_loop(0, n, lambda i, c: (body(i), c)[1], 0)


def of_head(shape, dim, head):
    return (iota(shape, dim) & HEAD_DIM) == head * HEAD_DIM


def centre(v):
    mean = jnp.mean(v, axis=-1, keepdims=True)
    off = v - mean
    rstd = lax.rsqrt(jnp.mean(off * off, axis=-1, keepdims=True) + EPS)
    return off * rstd, rstd


def centre_back(grad, hat, rstd, gain):
    scaled = grad * gain
    first = jnp.mean(scaled, axis=-1, keepdims=True)
    second = jnp.mean(scaled * hat, axis=-1, keepdims=True)
    return rstd * (scaled - first - hat * second)


def gelu_and_slope(u):
    bell = jnp.exp(-0.5 * u * u)
    t = 1.0 / (1.0 + (0.3275911 * 0.7071067811865476) * jnp.abs(u))
    poly = 0.5 * 1.061405429
    for c in (-1.453152027, 1.421413741, -0.284496736, 0.254829592):
        poly = poly * t + 0.5 * c
    tail = poly * t * bell
    cdf = jnp.where(u >= 0, 1.0 - tail, tail)
    return u * cdf, cdf + (0.3989422804014327 * u) * bell


def features_of(rows, wf):
    wide = rows.astype(F32)
    both = jnp.concatenate([rows, ((0.5 * FACTOR) * wide * wide).astype(BF16)], axis=1)
    return (jnp.exp(FACTOR * nn(both, wf)) * FEATURES ** (-0.5)).astype(BF16)


def features_back(rows, wf, weighted):
    through = nt(weighted, wf)
    half = 2 * HEAD_DIM
    return FACTOR * through[:, :half] + (FACTOR * FACTOR) * through[:, half:] * rows.astype(F32)


def with_ones(values):
    return jnp.concatenate([values, jnp.ones_like(values)], axis=1)


def merge_heads(state):
    own = of_head((state.shape[0], FEATURES), 0, 0)
    return jnp.where(own, state[:, :FEATURES], state[:, FEATURES:])


class Phases:
    def __init__(self, **refs):
        self.__dict__.update(refs)

    def set_up(self):
        fresh, last = self.fresh[...], self.last[...]
        zero = jnp.zeros((HEAD_DIM, FEATURES), BF16)
        minus = jnp.full((HEAD_DIM, FEATURES), -1.0, BF16)
        for j in range(PAIRS):
            for head in range(2):
                flag = (self.flags[2 * j + head] == 1).astype(F32)
                omega = (flag * fresh.astype(F32) + (1.0 - flag) * last.astype(F32)).astype(BF16)
                for lower, block in ((0, omega), (128, minus)):
                    for other in range(2):
                        at = pl.ds(lower + head * HEAD_DIM, HEAD_DIM)
                        col = pl.ds(other * FEATURES, FEATURES)
                        self.wf[j, at, col] = block if other == head else zero
        self.small[...] = jnp.zeros(self.small.shape, F32)

    def norm1(self):
        def body(t):
            at = row_tile(t, 128)
            hat, _ = centre(self.tokens[at, :].astype(F32))
            self.n1[at, :] = (hat * self.gains[0:1, :] + self.shifts[0:1, :]).astype(BF16)

        loop(ROWS // 128, body)

    def project(self, hh):
        for jj in range(2):
            self.run[jj] = jnp.zeros((TILE, FEATURES), F32)

        def body(t):
            rows = self.n1[row_tile(t), :]
            parts = [
                nn(rows, self.wqkv[hh, c]).astype(BF16) for c in range(3)
            ]
            for jj in range(2):
                j = 2 * hh + jj
                q, k, v = (p[:, jj * 128 : (jj + 1) * 128] for p in parts)
                self.q[j, row_tile(t), :] = q
                self.k[j, row_tile(t), :] = k
                self.vx[j, row_tile(t), :] = v
                wf = self.wf[j]
                self.phi_q[j, row_tile(t), :] = features_of(q, wf)
                phi_k = features_of(k, wf)
                self.phi_k[j, row_tile(t), :] = phi_k
                state = merge_heads(tn(with_ones(v), phi_k))
                self.zt[j * TILES + t] = state.astype(BF16)
                self.run[jj] += state

        loop(TILES, body)
        for jj in range(2):
            self.pack(self.zsend, 2 * hh + jj, self.run.at[jj], False)

    def pack(self, out, j, state, gradient):
        first, second = state[128:136, :], state[192:200, :]
        if gradient:
            first = 0.5 * (first + state[160:168, :])
            second = 0.5 * (second + state[224:232, :])
        out[j, 0:128, :] = state[0:128, :].astype(BF16)
        out[j, 128:136, :] = first.astype(BF16)
        out[j, 136:144, :] = second.astype(BF16)

    def unpack(self, packed):
        low = packed.astype(F32)
        sums = [jnp.broadcast_to(low[r : r + 1], (HEAD_DIM, FEATURES)) for r in (128, 136)]
        return jnp.concatenate([low[0:128], *sums], axis=0)

    def attend_near(self, hh):
        def body(t):
            at = row_tile(t)
            for j in (2 * hh, 2 * hh + 1):
                vx = with_ones(self.vx[j, at, :])
                both = []
                for head in range(2):
                    f = slice(head * FEATURES, (head + 1) * FEATURES)
                    s = nt(self.phi_q[j, at, f], self.phi_k[j, at, f])
                    s = jnp.where(iota(s.shape, 1) <= iota(s.shape, 0), s, 0.0).astype(BF16)
                    both.append(nn(s, vx))
                r = jnp.where(of_head(both[0].shape, 1, 0), both[0], both[1])
                self.out[at, lane_tile(j)] = r[:, :128]
                self.grad[at, lane_tile(j)] = r[:, 128:]

        loop(TILES, body)

    def attend_far(self, hh, start):
        for jj in range(2):
            self.run[jj] = start(2 * hh + jj)

        def body(t):
            at = row_tile(t)
            for jj in range(2):
                j = 2 * hh + jj
                before = self.run[jj]
                low = before.astype(BF16)
                self.run[jj] = before + self.zt[j * TILES + t].astype(F32)
                self.zt[j * TILES + t] = low
                both = [
                    nt(self.phi_q[j, at, head * FEATURES : (head + 1) * FEATURES], low)
                    for head in range(2)
                ]
                r = jnp.where(of_head(both[0].shape, 1, 0), both[0], both[1])
                inverse = 1.0 / (r[:, 128:] + self.grad[at, lane_tile(j)])
                num = r[:, :128] + self.out[at, lane_tile(j)]
                self.a[at, lane_tile(j)] = (num * inverse).astype(BF16)
                self.inverse[j, at, :] = inverse

        loop(TILES, body)

    def norm2(self):
        def body(t):
            at = row_tile(t)
            w_out = self.wout[...].reshape(WIDE, WIDE)
            h = self.tokens[at, :].astype(F32) + nn(self.a[at, :], w_out)
            self.out[at, :] = h
            hat, rstd = centre(h)
            self.hat2[at, :] = hat.astype(BF16)
            self.rstd2[at, :] = jnp.broadcast_to(rstd, (TILE, 128))
            self.n2[at, :] = (hat * self.gains[1:2, :] + self.shifts[1:2, :]).astype(BF16)
            self.grad[at, :] = jnp.zeros((TILE, WIDE), F32)

        loop(TILES, body)

    def feed_in(self, step, me):
        at, cols, slot, place = self.feed_place(step, me)
        g, slope = gelu_and_slope(nn(self.n2[at, :], self.wup[slot, :, cols]))
        self.g[place] = g.astype(BF16)
        self.du[place] = (slope * nt(self.cot[at, :], self.wdown[slot, cols, :])).astype(BF16)

    def feed_back(self, step, me):
        at, cols, slot, place = self.feed_place(step, me)
        self.grad[at, :] += nt(self.du[place], self.wup[slot, :, cols])

    def feed_place(self, step, me):
        late = lax.div(step, 2 * TILES)
        slot = me + late * (1 - 2 * me)
        t, p = lax.div(lax.rem(step, 2 * TILES), 2), lax.rem(step, 2)
        return row_tile(t), lane_tile(p, 512), slot, t * 4 + slot * 2 + p

    def feed(self, first, count, me):
        def body(n):
            self.feed_back(first + n - 1, me)
            self.feed_in(first + n, me)

        loop(count, body)

    def feed_out(self):
        def body(t):
            total = self.out[row_tile(t), :]
            for n in range(4):
                w_down = self.wdown[n // 2, (n % 2) * 512 : (n % 2) * 512 + 512, :]
                total = total + nn(self.g[t * 4 + n], w_down)
            self.out[row_tile(t), :] = total

        loop(TILES, body)

    def norm2_back(self):
        def body(t):
            at = row_tile(t, 128)
            grad, hat = self.grad[at, :], self.hat2[at, :].astype(F32)
            self.small[1:2, :] += jnp.sum(grad * hat, axis=0, keepdims=True)
            self.small[3:4, :] += jnp.sum(grad, axis=0, keepdims=True)
            back = centre_back(grad, hat, self.rstd2[at, 0:1], self.gains[1:2, :])
            dh = self.cot[at, :].astype(F32) + back
            self.grad[at, :] = dh
            self.dhb[at, :] = dh.astype(BF16)

        loop(ROWS // 128, body)

    def flip(self, source, out):
        def body(t):
            out[:, row_tile(t)] = source[row_tile(t), :].T

        loop(TILES, body)

    def weight_grad(self, xt, blocks, n_cols, store):
        def body(i):
            for c in (2 * i, 2 * i + 1):
                total = nn(xt[:, 0:TILE], blocks(0, c))
                for t in range(1, TILES):
                    total = total + nn(xt[:, t * TILE : (t + 1) * TILE], blocks(t, c))
                store(c, total)

        loop(n_cols // 2, body)

    def attend_back_start(self):
        def body(t):
            at = row_tile(t)
            w_out = self.wout[...].reshape(WIDE, WIDE)
            da = nt(self.dhb[at, :], w_out)
            o = self.a[at, :].astype(F32)
            same = (iota((128, 128), 0) & HEAD_DIM) == (iota((128, 128), 1) & HEAD_DIM)
            ones = jnp.where(same, 1.0, 0.0).astype(BF16)
            high = (iota((TILE, 128), 1) & 32) == 0
            for j in range(PAIRS):
                lanes = slice(j * 128, (j + 1) * 128)
                do, inverse = da[:, lanes], self.inverse[j, at, :]
                dden = -nn((do * o[:, lanes]).astype(BF16), ones) * inverse
                top = dden.astype(BF16)
                rest = (dden - top.astype(F32)).astype(BF16)
                self.dnx[j, at, 0:128] = (do * inverse).astype(BF16)
                self.dnx[j, at, 128:] = jnp.where(high, top, rest) * jnp.asarray(1 / 32, BF16)

        loop(TILES, body)

    def sums_back(self, j):
        total = jnp.zeros((TILE, FEATURES), F32)
        for t in range(TILES):
            at = slice(t * TILE, (t + 1) * TILE)
            state = merge_heads(tn(self.dnx[j, at, :], self.phi_q[j, at, :]))
            self.gt[j * TILES + t] = state.astype(BF16)
            total = total + state
        self.run[0] = total
        self.pack(self.gsend, j, self.run.at[0], True)

    def back_q(self, j):
        def body(i):
            for t in (2 * i, 2 * i + 1):
                at = row_tile(t)
                dnx = self.dnx[j, at, :]
                w = []
                for head in range(2):
                    f = slice(head * FEATURES, (head + 1) * FEATURES)
                    own = jnp.where(of_head(dnx.shape, 1, head), dnx, jnp.zeros_like(dnx))
                    ds = nt(own, with_ones(self.vx[j, at, :]))
                    ds = jnp.where(iota(ds.shape, 1) <= iota(ds.shape, 0), ds, 0.0).astype(BF16)
                    dphi = nn(ds, self.phi_k[j, at, f]) + nn(own, self.zt[j * TILES + t])
                    w.append((dphi * self.phi_q[j, at, f].astype(F32)).astype(BF16))
                dq = features_back(self.q[j, at, :], self.wf[j], jnp.concatenate(w, axis=1))
                self.dqkv[0 * TILES + t, :, lane_tile(j)] = dq.astype(BF16)

        loop(TILES // 2, body)

    def back_kv(self, j, start):
        self.run[0] = start(j)

        def body(i):
            t = TILES - 1 - i
            at = row_tile(t)
            after = self.run[0]
            low = after.astype(BF16)
            self.run[0] = after + self.gt[j * TILES + t].astype(F32)
            dnx, vx = self.dnx[j, at, :], with_ones(self.vx[j, at, :])
            w, dv = [], []
            for head in range(2):
                f = slice(head * FEATURES, (head + 1) * FEATURES)
                phi_q, phi_k = self.phi_q[j, at, f], self.phi_k[j, at, f]
                st = nt(phi_k, phi_q)
                upper = iota(st.shape, 0) <= iota(st.shape, 1)
                st = jnp.where(upper, st, 0.0).astype(BF16)
                own = jnp.where(of_head(vx.shape, 1, head), vx, jnp.zeros_like(vx))
                dst = nt(own, dnx)
                dst = jnp.where(upper, dst, 0.0).astype(BF16)
                dphi = nn(dst, phi_q) + nn(own, low)
                w.append((dphi * phi_k.astype(F32)).astype(BF16))
                dv.append(nn(st, dnx[:, 0:128]) + nt(phi_k, low[0:128]))
            dk = features_back(self.k[j, at, :], self.wf[j], jnp.concatenate(w, axis=1))
            self.dqkv[1 * TILES + t, :, lane_tile(j)] = dk.astype(BF16)
            dv = jnp.where(of_head(dv[0].shape, 1, 0), dv[0], dv[1])
            self.dqkv[2 * TILES + t, :, lane_tile(j)] = dv.astype(BF16)

        loop(TILES, body)

    def norm1_back(self, first, count):
        def body(n):
            t = first + n
            at = row_tile(t)
            grad = jnp.zeros((TILE, WIDE), F32)
            for hh in range(2):
                for c in range(3):
                    part = self.dqkv[c * TILES + t, :, hh * 256 : (hh + 1) * 256]
                    grad = grad + nt(part, self.wqkv[hh, c])
            hat, rstd = centre(self.tokens[at, :].astype(F32))
            self.small[0:1, :] += jnp.sum(grad * hat, axis=0, keepdims=True)
            self.small[2:3, :] += jnp.sum(grad, axis=0, keepdims=True)
            self.grad[at, :] += centre_back(grad, hat, rstd, self.gains[0:1, :])

        loop(count, body)


def work_buffers():
    vmem = pltpu.VMEM
    return dict(
        n1=vmem((ROWS, WIDE), BF16),
        q=vmem((PAIRS, ROWS, 128), BF16),
        k=vmem((PAIRS, ROWS, 128), BF16),
        vx=vmem((PAIRS, ROWS, 128), BF16),
        phi_q=vmem((PAIRS, ROWS, 512), BF16),
        phi_k=vmem((PAIRS, ROWS, 512), BF16),
        zt=vmem((PAIRS * TILES, 256, 256), BF16),
        gt=vmem((PAIRS * TILES, 256, 256), BF16),
        run=vmem((2, 256, 256), F32),
        wf=vmem((PAIRS, 256, 512), BF16),
        a=vmem((ROWS, WIDE), BF16),
        inverse=vmem((PAIRS, ROWS, 128), F32),
        n2=vmem((ROWS, WIDE), BF16),
        hat2=vmem((ROWS, WIDE), BF16),
        rstd2=vmem((ROWS, 128), F32),
        g=vmem((TILES * 4, 256, 512), BF16),
        du=vmem((TILES * 4, 256, 512), BF16),
        dnx=vmem((PAIRS, ROWS, 256), BF16),
        zsend=vmem((PAIRS, 144, 256), BF16),
        gsend=vmem((PAIRS, 144, 256), BF16),
        xt=vmem((WIDE, ROWS), BF16),
        xt2=vmem((WIDE, ROWS), BF16),
    )


MESH = pl.DeviceIdType.MESH
OWNED = 1024


class Links:
    def __init__(self, deep, refs):
        self.deep = deep
        self.__dict__.update(refs)
        self.dp, self.me = lax.axis_index("dp"), lax.axis_index("tensor")
        self.core = lax.rem(self.dp, 2)
        self.x = lax.rem(lax.div(self.dp, 2), 2)
        self.z = lax.div(self.dp, 4)
        self.block = WIDE // (4 * deep)

    def place(self, axis, step=1):
        dp, me = self.dp, self.me
        if axis == "core":
            return dict(dp=dp + 1 - 2 * self.core, tensor=me)
        if axis == "x":
            return dict(dp=dp + 2 - 4 * self.x, tensor=me)
        if axis == "y":
            return dict(dp=dp, tensor=1 - me)
        return dict(dp=dp + 4 * (lax.rem(self.z + step, self.deep) - self.z), tensor=me)

    def partners(self):
        steps = [self.place("z", s) for s in range(1, self.deep)]
        return [self.place(a) for a in ("core", "x", "y")] + steps

    def greet(self):
        barrier = pltpu.get_barrier_semaphore()
        for where in self.partners():
            pl.semaphore_signal(barrier, inc=1, device_id=where, device_id_type=MESH)

    def met(self):
        pl.semaphore_wait(pltpu.get_barrier_semaphore(), len(self.partners()))

    def copy(self, source, target, sems, at, where):
        return pltpu.make_async_remote_copy(
            src_ref=source,
            dst_ref=target,
            send_sem=sems.at[2 * at],
            recv_sem=sems.at[2 * at + 1],
            device_id=where,
            device_id_type=MESH,
        )


    def parts(self, i):
        if i < 3:
            source, slots = self.wqkv_in.at[i], [self.wqkv.at[t, i] for t in (self.me, 1 - self.me)]
        else:
            source = (self.wout_in, self.wup_in, self.wdown_in)[i - 3]
            whole = (self.wout, self.wup, self.wdown)[i - 3]
            slots = [whole.at[t] for t in (self.me, 1 - self.me)]
        size = source.shape[-2] // (2 if i < 4 else 4)

        def cut(ref, p):
            return ref.at[pl.ds(pl.multiple_of(p * size, size), size)]

        return source, *slots, cut

    def part(self, i, far=False):
        if i < 4:
            return self.core
        return 2 * ((1 - self.x) if far else self.x) + self.core

    def own_weight(self, i):
        source, mine, _, _ = self.parts(i)
        return pltpu.make_async_copy(source, mine, self.own_sems.at[i])

    def over(self, i):
        source, mine, _, cut = self.parts(i)
        p = self.part(i)
        return self.copy(cut(source, p), cut(mine, p), self.over_sems, i, self.place("y"))

    def across(self, i):
        _, _, other, cut = self.parts(i)
        held = cut(other, self.part(i))
        return self.copy(held, held, self.across_sems, i - 4, self.place("x"))

    def along(self, i, far=False):
        _, _, other, cut = self.parts(i)
        held = cut(other, self.part(i, far))
        return self.copy(held, held, self.along_sems, i + (2 if far else 0), self.place("core"))


    def axes(self, seg):
        return ("y", "x") if seg % 2 == 0 else ("x", "y")

    def index(self, axis):
        return self.me if axis == "y" else self.x

    def stage(self, seg, depth):
        grads = self.grads[seg]
        if depth == 0:
            source = grads.at[1 - self.core]
            return self.copy(source, self.got[seg][0], self.sum_sems[seg], 0, self.place("core"))
        axis = self.axes(seg)[depth - 1]
        start, size = self.span(seg, depth, 1 - self.index(axis))
        source = grads.at[self.core, pl.ds(pl.multiple_of(start, self.block), size)]
        return self.copy(source, self.got[seg][depth], self.sum_sems[seg], depth, self.place(axis))

    def span(self, seg, depth, last):
        start, size = 0, WIDE
        for i in range(depth):
            size = size // 2
            at = last if i == depth - 1 else self.index(self.axes(seg)[i])
            start = start + at * size
        return start, size

    def mine(self, seg, depth):
        if depth == 0:
            return 0, WIDE
        return self.span(seg, depth, self.index(self.axes(seg)[depth - 1]))

    def start(self, seg, depth):
        self.stage(seg, depth).start()

    def finish(self, seg, depth):
        self.stage(seg, depth).wait()
        start, size = self.mine(seg, depth)
        grads, got = self.grads[seg], self.got[seg][depth]
        step = min(size, 64)

        def body(i):
            there = pl.ds(pl.multiple_of(i * step, step), step)
            here = pl.ds(pl.multiple_of(start + i * step, step), step)
            grads[self.core, here] = grads[self.core, here] + got[there]

        loop(size // step, body)

    def z_copy(self, seg, step):
        start, _ = self.mine(seg, 2)
        row = start + lax.rem(self.z + step, self.deep) * self.block
        source = self.grads[seg].at[self.core, pl.ds(pl.multiple_of(row, self.block), self.block)]
        target = self.got[seg][3].at[step - 1]
        return self.copy(source, target, self.sum_sems[seg], 2 + step, self.place("z", step))

    def start_z(self, seg):
        for step in range(1, self.deep):
            self.z_copy(seg, step).start()

    def finish_z(self, seg):
        start, _ = self.mine(seg, 2)
        here = pl.ds(pl.multiple_of(start + self.z * self.block, self.block), self.block)
        total = self.grads[seg][self.core, here].astype(F32)
        for step in range(1, self.deep):
            self.z_copy(seg, step).wait()
            total = total + self.got[seg][3][step - 1].astype(F32)
        return total


    def small_copies(self, stage):
        if stage < 3:
            places = [self.place(("core", "y", "x")[stage])]
        else:
            places = [self.place("z", s) for s in range(1, self.deep)]
        return [
            self.copy(self.small.at[stage], self.heard.at[stage + n], self.small_sems, stage + n, where)
            for n, where in enumerate(places)
        ]

    def small_start(self, stage):
        for both in self.small_copies(stage):
            both.start()

    def small_finish(self, stage):
        total = self.small[stage]
        for n, both in enumerate(self.small_copies(stage)):
            both.wait()
            total = total + self.heard[stage + n]
        self.small[stage + 1] = total


def by_owner(ref, flipped, deep, total, tensor, lanes):
    block = WIDE // (4 * deep)
    low = total.astype(BF16)
    for d in range(4 * deep):
        core, x, z = d % 2, d // 2 % 2, d // 4
        near, far = (x, tensor) if flipped else (tensor, x)
        row = ((near * 2 + far) * deep + z) * block
        here = pl.ds(pl.multiple_of(row, block), block)
        ref[core, here, lanes] = low[d * block : (d + 1) * block]


def layer_kernel(deep, names, *refs):
    r = dict(zip(names, refs))
    sends = r["sum_sems"]
    links = Links(
        deep,
        dict(
            r,
            grads=tuple(r[f"grads{s}"] for s in range(4)),
            got=tuple(tuple(r[f"got{s}_{d}"] for d in range(4)) for s in range(4)),
            sum_sems=tuple(sends.at[s] for s in range(4)),
        ),
    )
    p = Phases(**dict(r, dqkv=r["du"], dhb=r["hat2"], small=r["small"].at[0]))
    me = links.me
    other = 1 - me

    links.greet()
    for i in range(6):
        links.own_weight(i).start()
    cot_in = pltpu.make_async_copy(r["cot_in"], p.cot, r["io_sems"].at[0])
    cot_in.start()
    p.set_up()
    links.met()
    for i in range(4):
        links.over(i).start()
    p.norm1()
    for i in range(3):
        links.own_weight(i).wait()
    p.project(me)

    def z_copy(hh):
        here = pl.ds(2 * hh, 2)
        return links.copy(p.zsend.at[here], p.zgot.at[here], r["z_sems"], hh, links.place("y"))

    @pl.when(me == 0)
    def _():
        p.zgot[...] = jnp.zeros(p.zgot.shape, BF16)
        z_copy(0).start()

    @pl.when(me == 1)
    def _():
        p.ggot[...] = jnp.zeros(p.ggot.shape, BF16)

    links.over(4).start()
    p.attend_near(me)
    for i in range(3):
        links.over(i).wait()
        links.along(i).start()
    for i in range(3):
        links.along(i).wait()
    p.project(other)

    @pl.when(me == 0)
    def _():
        z_copy(1).start()

    links.over(5).start()
    links.over(3).wait()
    links.along(3).start()
    p.attend_near(other)
    links.over(4).wait()
    links.across(4).start()
    links.along(4).start()
    for hh in range(2):

        @pl.when(me == 1)
        def _():
            z_copy(hh).wait_recv()

        p.attend_far(hh, lambda j: p.unpack(p.zgot[j]))

        @pl.when(me == 0)
        def _():
            z_copy(hh).wait_send()

    links.own_weight(3).wait()
    links.along(3).wait()
    p.norm2()
    links.own_weight(4).wait()
    links.own_weight(5).wait()
    cot_in.wait()
    p.feed_in(0, me)
    p.feed(1, 3, me)
    links.across(4).wait()
    links.along(4, True).start()
    links.over(5).wait()
    links.across(5).start()
    links.along(5).start()
    p.feed(4, 4, me)
    links.across(5).wait()
    links.along(5, True).start()
    for i in range(4, 6):
        links.along(i).wait()
        links.along(i, True).wait()
    p.feed(8, 8, me)
    p.feed_back(15, me)

    p.norm2_back()
    p.attend_back_start()
    loop(PAIRS, p.sums_back)
    g_copy = links.copy(p.gsend, p.ggot, r["g_sems"], 0, links.place("y"))

    @pl.when(me == 1)
    def _():
        g_copy.start()

    def ff_grad(xt, blocks, seg):
        def store(c, total):
            lanes = lane_tile(lax.rem(c, 4), TILE)
            by_owner(links.grads[seg], seg == 1, deep, total, lax.div(c, 4), lanes)

        def take(t, c):
            return blocks[t * 4 + lax.div(c, 2), :, lane_tile(lax.rem(c, 2), TILE)]

        p.weight_grad(xt, take, 8, store)

    p.flip(p.n2, p.xt)
    ff_grad(p.xt, p.du, 0)
    links.start(0, 0)
    p.flip(p.cot, p.xt2)
    ff_grad(p.xt2, p.g, 1)
    links.start(1, 0)
    p.flip(p.dhb, p.xt)
    p.weight_grad(
        p.xt,
        lambda t, c: p.a[pl.ds(t * TILE, TILE), lane_tile(c, TILE)],
        2,
        lambda c, total: by_owner(links.grads[2], False, deep, total, c, slice(0, TILE)),
    )
    p.flip(p.n1, p.xt2)
    links.finish(0, 0)
    links.start(0, 1)
    loop(2, p.back_q)
    links.finish(1, 0)
    links.start(1, 1)
    loop(2, lambda j: p.back_q(j + 2))

    @pl.when(me == 0)
    def _():
        g_copy.wait_recv()

    @pl.when(me == 1)
    def _():
        g_copy.wait_send()

    def back(j):
        p.back_kv(j, lambda j: p.unpack(p.ggot[j]))

    def qkv_grad(seg):
        pieces = [(hh, c) for hh in range(2) for c in range(3)]
        base = (0, 0, TILE, 0)[seg]
        for n in range(3):
            total = jnp.zeros((WIDE, TILE), F32)
            for t in range(TILES):
                rows = [
                    p.dqkv[c * TILES + t, :, lane_tile(2 * hh + seg - 2)]
                    for hh, c in pieces[2 * n : 2 * n + 2]
                ]
                total = total + nn(
                    p.xt2[:, t * TILE : (t + 1) * TILE], jnp.concatenate(rows, axis=1)
                )
            for half, (hh, c) in enumerate(pieces[2 * n : 2 * n + 2]):
                by_owner(
                    links.grads[seg],
                    seg == 3,
                    deep,
                    total[:, half * 128 : (half + 1) * 128],
                    hh,
                    pl.ds(base + c * 128, 128),
                )

    back(0)
    for seg in range(2):
        links.finish(seg, 1)
        links.start(seg, 2)
    back(2)
    qkv_grad(2)
    links.start(2, 0)
    back(1)
    links.finish(2, 0)
    links.start(2, 1)
    for seg in range(2):
        links.finish(seg, 2)
        links.start_z(seg)
    back(3)
    qkv_grad(3)
    links.start(3, 0)
    p.norm1_back(0, 2)
    links.finish(3, 0)
    links.start(3, 1)
    p.norm1_back(2, 2)
    grad_copy = pltpu.make_async_copy(p.grad, r["grad_hbm"], r["io_sems"].at[2])
    grad_copy.start()
    links.small_start(0)
    links.finish(2, 1)
    links.start(2, 2)
    p.feed_out()
    out_copy = pltpu.make_async_copy(p.out, r["out_hbm"], r["io_sems"].at[1])
    out_copy.start()
    r["own_up"][...] = links.finish_z(0)
    r["own_down"][...] = links.finish_z(1)
    links.small_finish(0)
    links.small_start(1)
    links.finish(3, 1)
    links.start(3, 2)
    links.small_finish(1)
    links.small_start(2)
    links.finish(2, 2)
    links.start_z(2)
    links.finish(3, 2)
    links.start_z(3)
    links.small_finish(2)
    links.small_start(3)

    def own_qkv(total, jj):
        for c in range(3):
            r["own_qkv"][c, :, jj * 128 : (jj + 1) * 128] = total[:, c * 128 : (c + 1) * 128]

    total = links.finish_z(2)
    r["own_wout"][...] = total[:, :TILE]
    own_qkv(total[:, TILE:], 0)
    own_qkv(links.finish_z(3), 1)
    links.small_finish(3)
    r["own_gains"][...] = r["small"][4, 0:2]
    r["own_shifts"][...] = r["small"][4, 2:4]
    out_copy.wait()
    grad_copy.wait()


def layer_call(deep, tokens, cotangent, wqkv, wout, wup, wdown, gains, shifts, fresh, last, flags):
    vmem, hbm = pltpu.VMEM, pl.ANY
    block = WIDE // (4 * deep)
    inputs = dict(
        tokens=(tokens, vmem),
        cot_in=(cotangent, hbm),
        wqkv_in=(wqkv, hbm),
        wout_in=(wout, hbm),
        wup_in=(wup, hbm),
        wdown_in=(wdown, hbm),
        gains=(gains, vmem),
        shifts=(shifts, vmem),
        fresh=(fresh, vmem),
        last=(last, vmem),
        flags=(flags, pltpu.SMEM),
    )
    outputs = dict(
        out_hbm=((ROWS, WIDE), hbm),
        grad_hbm=((ROWS, WIDE), hbm),
        own_qkv=((3, block, 256), vmem),
        own_wout=((block, 256), vmem),
        own_up=((block, 1024), vmem),
        own_down=((block, 1024), vmem),
        own_gains=((2, WIDE), vmem),
        own_shifts=((2, WIDE), vmem),
    )
    dma = pltpu.SemaphoreType.DMA
    widths = (1024, 1024, 640, 384)
    scratch = dict(
        work_buffers(),
        out=vmem((ROWS, WIDE), F32),
        grad=vmem((ROWS, WIDE), F32),
        cot=vmem((ROWS, WIDE), BF16),
        wqkv=vmem((2, 3, WIDE, 256), BF16),
        wout=vmem((2, 256, WIDE), BF16),
        wup=vmem((2, WIDE, 1024), BF16),
        wdown=vmem((2, 1024, WIDE), BF16),
        zgot=vmem((PAIRS, 144, 256), BF16),
        ggot=vmem((PAIRS, 144, 256), BF16),
        small=vmem((5, 4, WIDE), F32),
        heard=vmem((2 + deep, 4, WIDE), F32),
        own_sems=dma((6,)),
        over_sems=dma((12,)),
        across_sems=dma((4,)),
        along_sems=dma((16,)),
        z_sems=dma((4,)),
        g_sems=dma((2,)),
        io_sems=dma((3,)),
        sum_sems=dma((4, 2 * (2 + deep))),
        small_sems=dma((2 * (2 + deep),)),
    )
    for seg, width in enumerate(widths):
        scratch[f"grads{seg}"] = vmem((2, WIDE, width), BF16)
        for depth in range(3):
            scratch[f"got{seg}_{depth}"] = vmem((WIDE // 2**depth, width), BF16)
        scratch[f"got{seg}_3"] = vmem((deep - 1, block, width), BF16)
    names = (*inputs, *outputs, *scratch)

    def kernel(*refs):
        layer_kernel(deep, names, *refs)

    return pl.pallas_call(
        kernel,
        out_shape=tuple(jax.ShapeDtypeStruct(shape, F32) for shape, _ in outputs.values()),
        in_specs=[pl.BlockSpec(memory_space=space) for _, space in inputs.values()],
        out_specs=tuple(pl.BlockSpec(memory_space=space) for _, space in outputs.values()),
        scratch_shapes=list(scratch.values()),
        compiler_params=pltpu.CompilerParams(
            collective_id=0, has_side_effects=True, vmem_limit_bytes=67043328
        ),
        name="layer",
    )(*(array for array, _ in inputs.values()))


def hand_over(arrays):
    count = len(arrays)

    def kernel(*refs):
        ins, outs, held = refs[:count], refs[count : 2 * count], refs[2 * count : 3 * count]
        sems = refs[3 * count]
        pieces = []
        for i, array in enumerate(arrays):
            cuts = 4 if array.shape[0] == ROWS else 1
            size = array.shape[0] // cuts
            for n in range(cuts):
                here = pl.ds(n * size, size)
                at = len(pieces)
                fetch = pltpu.make_async_copy(ins[i].at[here], held[i].at[here], sems.at[0, at])
                store = pltpu.make_async_copy(held[i].at[here], outs[i].at[here], sems.at[1, at])
                pieces.append((fetch, store))
        for fetch, _ in pieces:
            fetch.start()
        for fetch, store in pieces:
            fetch.wait()
            store.start()
        for _, store in pieces:
            store.wait()

    anywhere = pl.BlockSpec(memory_space=pl.ANY)
    return pl.pallas_call(
        kernel,
        out_shape=tuple(jax.ShapeDtypeStruct(a.shape, a.dtype) for a in arrays),
        in_specs=[anywhere] * count,
        out_specs=(anywhere,) * count,
        scratch_shapes=[pltpu.VMEM(a.shape, a.dtype) for a in arrays]
        + [pltpu.SemaphoreType.DMA((2, 16))],
        name="hand_over",
    )(*arrays)


def fused(
    tokens, cotangent, w_qkv, w_out, w_up, w_down, gains, shifts, feat_fresh, feat_last, flags
):
    deep = lax.axis_size("dp") // 4
    by_part = jnp.transpose(w_qkv, (1, 0, 2))
    outs = hand_over(layer_call(
        deep,
        tokens,
        cotangent,
        by_part,
        w_out,
        w_up,
        w_down,
        gains,
        shifts,
        feat_fresh,
        feat_last,
        flags,
    ))
    result, grad_tokens, own_qkv, own_wout, own_up, own_down, own_gains, own_shifts = outs
    return (
        result,
        grad_tokens,
        jnp.transpose(own_qkv, (1, 0, 2)),
        own_wout.T,
        own_up,
        own_down.T,
        own_gains,
        own_shifts,
    )


def fits(mesh):
    return mesh.shape["tensor"] == 2 and mesh.shape["dp"] % 4 == 0 and mesh.shape["dp"] <= 64


def normalize(inputs, norm_gain, offset):
    average = jnp.mean(inputs, axis=-1, keepdims=True)
    centered = inputs - average
    variance = jnp.mean(centered * centered, axis=-1, keepdims=True)
    return centered * lax.rsqrt(variance + EPS) * norm_gain + offset


def gelu_exact(inputs):
    return jax.nn.gelu(inputs, approximate=False)


def mul(spec, *operands):
    return jnp.einsum(spec, *operands, preferred_element_type=F32)


def split_heads(matrix):
    length = matrix.shape[0]
    return jnp.transpose(matrix.reshape(length, -1, HEAD_DIM), (1, 0, 2))


def join_heads(stacked):
    moved = jnp.transpose(stacked, (1, 0, 2))
    return moved.reshape(moved.shape[0], -1)


def plain_features(inputs, projector):
    factor = HEAD_DIM ** (-0.25)
    projected = mul("hlc,hcm->hlm", inputs, projector)
    wide_in = inputs.astype(F32)
    squares = 0.5 * factor * factor * jnp.sum(wide_in * wide_in, axis=-1, keepdims=True)
    return jnp.exp(factor * projected - squares) * FEATURES ** (-0.5)


def plain_features_back(inputs, projector, expo, grad_phi):
    factor = HEAD_DIM ** (-0.25)
    grad_pre = grad_phi * expo
    grad_proj = (factor * grad_pre).astype(BF16)
    through = mul("hlm,hcm->hlc", grad_proj, projector)
    return through - factor * factor * jnp.sum(grad_pre, axis=-1, keepdims=True) * inputs.astype(F32)


def from_others(part, before):
    parts = lax.all_gather(part, "tensor")
    mine = lax.axis_index("tensor")
    place = jnp.arange(parts.shape[0])
    taken = (place < mine) if before else (place > mine)
    return jnp.sum(jnp.where(taken[:, None, None, None], parts, 0.0), axis=0)


def with_sums(values):
    return jnp.concatenate([values, jnp.ones_like(values[..., :1])], axis=-1)


def plain(
    tokens, cotangent, w_qkv, w_out, w_up, w_down, gains, shifts, feat_fresh, feat_last, flags
):
    w_qkv = lax.all_gather(w_qkv, "tensor", axis=2, tiled=True)
    w_out = lax.all_gather(w_out, "tensor", axis=0, tiled=True)
    w_up = lax.all_gather(w_up, "tensor", axis=1, tiled=True)
    w_down = lax.all_gather(w_down, "tensor", axis=0, tiled=True)
    inputs = tokens.astype(F32)
    rows = inputs.shape[0]
    normed, first_pull = jax.vjp(normalize, inputs, gains[0], shifts[0])
    normed = normed.astype(BF16)
    projector = jnp.where((flags == 1)[:, None, None], feat_fresh[None], feat_last[None])
    mixed = mul("ld,dce->cle", normed, w_qkv).astype(BF16)
    queries, keys, values = (split_heads(mixed[c]) for c in range(3))
    expo_q, expo_k = plain_features(queries, projector), plain_features(keys, projector)
    phi_q, phi_k = expo_q.astype(BF16), expo_k.astype(BF16)
    summed_values = with_sums(values)
    memory = from_others(mul("hkm,hke->hme", phi_k, summed_values), True).astype(BF16)
    causal = jnp.tril(jnp.ones((rows, rows), jnp.bool_))
    scores = jnp.where(causal, mul("hcm,hkm->hck", phi_q, phi_k), 0.0).astype(BF16)
    both = mul("hck,hke->hce", scores, summed_values) + mul("hcm,hme->hce", phi_q, memory)
    denoms = both[..., -1:]
    outputs = both[..., :-1] / denoms
    joined = join_heads(outputs).astype(BF16)
    residual = inputs + mul("le,ed->ld", joined, w_out)
    second, second_pull = jax.vjp(normalize, residual, gains[1], shifts[1])
    second = second.astype(BF16)
    pre_act = mul("ld,df->lf", second, w_up)
    activated, gelu_pull = jax.vjp(gelu_exact, pre_act)
    act_low = activated.astype(BF16)
    result = residual + mul("lf,fd->ld", act_low, w_down)
    grad_act = mul("ld,fd->lf", cotangent, w_down)
    grad_pre = gelu_pull(grad_act)[0].astype(BF16)
    grad_down = mul("ld,lf->df", cotangent, act_low)
    grad_up = mul("ld,lf->df", second, grad_pre)
    grad_resid, grad_gain2, grad_shift2 = second_pull(mul("lf,df->ld", grad_pre, w_up))
    grad_resid = grad_resid + cotangent.astype(F32)
    resid_low = grad_resid.astype(BF16)
    grad_out = split_heads(mul("ld,ed->le", resid_low, w_out))
    grad_wout = mul("ld,le->de", resid_low, joined)
    grad_num = (grad_out / denoms).astype(BF16)
    grad_den = -jnp.sum(grad_out * outputs, axis=-1, keepdims=True) / denoms
    grad_both = jnp.concatenate([grad_num, grad_den.astype(BF16)], axis=-1)
    grad_memory = from_others(mul("hcm,hce->hme", phi_q, grad_both), False).astype(BF16)
    grad_scores = jnp.where(
        causal, (mul("hce,hke->hck", grad_num, values) + grad_den).astype(BF16), 0
    )
    grad_q = mul("hck,hkm->hcm", grad_scores, phi_k) + mul("hce,hme->hcm", grad_both, memory)
    grad_k = mul("hck,hcm->hkm", grad_scores, phi_q)
    grad_k = grad_k + mul("hke,hme->hkm", summed_values, grad_memory)
    grad_v = mul("hck,hce->hke", scores, grad_num)
    grad_v = grad_v + mul("hkm,hme->hke", phi_k, grad_memory[..., :-1])
    grad_mixed = jnp.stack(
        [
            join_heads(plain_features_back(queries, projector, expo_q, grad_q)),
            join_heads(plain_features_back(keys, projector, expo_k, grad_k)),
            join_heads(grad_v),
        ]
    ).astype(BF16)
    grad_wqkv = mul("ld,cle->dce", normed, grad_mixed)
    grad_normed = mul("cle,dce->ld", grad_mixed, w_qkv)
    grad_inputs, grad_gain1, grad_shift1 = first_pull(grad_normed)
    grad_tokens = grad_resid + grad_inputs

    tensor, dp = lax.axis_size("tensor"), lax.axis_size("dp")
    wide = grad_wqkv.shape[0]

    def by_owner(grad):
        shaped = grad.reshape(dp, wide // dp, -1, tensor, grad.shape[-1] // tensor)
        moved = jnp.transpose(shaped, (0, 3, 1, 2, 4))
        return moved.reshape(dp * tensor, wide // dp, -1).astype(BF16)

    packed = jnp.concatenate(
        [by_owner(g) for g in (grad_wqkv, grad_wout, grad_up, grad_down)], axis=2
    )
    owned = lax.psum_scatter(packed, ("dp", "tensor"), scatter_dimension=0, tiled=True)[0]
    owned = owned.astype(F32)
    edge = [3 * wide // tensor, 4 * wide // tensor, 4 * wide // tensor + w_up.shape[1] // tensor]
    own_qkv, own_wout, own_up, own_down = jnp.split(owned, edge, axis=1)
    grad_gains, grad_shifts = lax.psum(
        (jnp.stack([grad_gain1, grad_gain2]), jnp.stack([grad_shift1, grad_shift2])),
        ("dp", "tensor"),
    )
    return (
        result,
        grad_tokens,
        own_qkv.reshape(wide // dp, 3, wide // tensor),
        own_wout.T,
        own_up,
        own_down.T,
        grad_gains,
        grad_shifts,
    )


def solution(mesh):
    placed = (
        P(("dp", "tensor"), None),
        P(("dp", "tensor"), None),
        P(None, None, "tensor"),
        P("tensor", None),
        P(None, "tensor"),
        P("tensor", None),
        P(),
        P(),
        P(),
        P(),
        P(),
    )
    return jax.shard_map(
        fused if fits(mesh) else plain,
        mesh=mesh,
        in_specs=placed,
        out_specs=(
            P(("dp", "tensor"), None),
            P(("dp", "tensor"), None),
            P("dp", None, "tensor"),
            P("tensor", "dp"),
            P("dp", "tensor"),
            P("tensor", "dp"),
            P(),
            P(),
        ),
        check_vma=False,
    )
```
